128 devices in a mesh: row: 8 (over z_hi, x), col: 16 (over z_lo, y, core).
Axes of the slice: x: 4, y: 4, z: 4 (z_hi: 2, z_lo: 2; z = z_hi * 2 + z_lo), core: 2. Of those that a mesh axis runs over, the one named last changes fastest.
Arguments:
- tokens: bfloat16 [16384, 2048], P(('row', 'col')), may hold values from -6 to 6
- expert_ids: int32 [16384, 8], P(('row', 'col')), may hold values from 0 to 127, all different within a row; in each aligned block of 128 rows (0 to 127, 128 to 255, ...) at most 10 rows name the same one
- gate_probs: float32 [16384, 8], P(('row', 'col')), may hold values from 0.05 to 0.5
- w_gate: bfloat16 [128, 2048, 768], P(('row', 'col')), may hold values from -0.125 to 0.125
- w_up: bfloat16 [128, 2048, 768], P(('row', 'col')), may hold values from -0.125 to 0.125
- w_down: bfloat16 [128, 768, 2048], P(('row', 'col')), may hold values from -0.21875 to 0.21875
Outputs:
- mixed: bfloat16 [16384, 2048], P(('row', 'col'))
The draws below stay inside these ranges and needn't reach their ends.
Inputs may be any that keep to these rules, and one draw needn't show every extreme that they name: `expert_ids`: each row names 8 different experts; among the rows of one device (aligned blocks of 128 rows) no expert is named more than 10 times.
All inputs are finite; a program needn't handle non-finite values.
Results may differ from the reference program's by a relative error of at most 0.0058.
Values may be sent and summed in bfloat16 or wider, within the bound.
A program may use at most 128 MiB of HBM per device.

```python
import math
import jax
import jax.numpy as jnp
import numpy as np
from jax import lax

D = 2048
FF = 768
TOPK = 8
TOK_DEV = 128
EXPERTS = 128
TOKENS = 16384
SLOTS = 10
N_ROW = 8
N_COL = 16


def level_of(stream_key, extent, shards, smallest, high):
    def one(axis_at, blocks):
        draws = jax.random.uniform(jax.random.fold_in(jax.random.fold_in(stream_key, 6), axis_at), (blocks,), jnp.float32, smallest / len(shards), high / len(shards))
        return jnp.repeat(jnp.exp(draws), extent[axis_at] // blocks).reshape((-1,) + (1,) * (len(extent) - axis_at - 1))

    loudness = one(*shards[0])
    for cut in shards[1:]:
        loudness = loudness * one(*cut)
    return loudness


def shared_out(own_key, own, number, rows, count, top, most, slope):
    order = jax.random.permutation(own_key, count)
    crowded, ordinary = load_shares(count, rows * top, most, slope, True), load_shares(count, rows * top, most, slope, False)
    places = jnp.arange(count)

    def named(lengths, rotation):
        used = int((lengths > 0).sum())
        fixed = max(1, used // 4)
        shifted = fixed + (places - fixed + rotation * (used - fixed)) % max(1, count - fixed)
        return jnp.zeros((count,), jnp.int32).at[order[jnp.where(places < fixed, places, shifted)]].set(jnp.asarray(lengths, jnp.int32))

    lengths = jnp.where(number % 4 == 0, named(crowded, number // 4), named(ordinary, number - number // 4 - 1))
    mixed = jax.random.permutation(jax.random.fold_in(own, 3), count)
    source_of, taker = mixed[0:count // 2 * 2:2], mixed[1:count // 2 * 2:2]
    room = jnp.minimum(lengths[source_of] - 1, most - lengths[taker]) // 2
    room = jnp.where((source_of == order[0]) | (taker == order[0]) | (lengths[taker] == 0), 0, jnp.maximum(room, 0))
    shifted = jax.random.randint(jax.random.fold_in(own, 4), (count // 2,), 0, 1 << 20) % (room + 1)
    lengths = lengths.at[source_of].add(-shifted).at[taker].add(shifted)
    members = jnp.searchsorted(jnp.cumsum(lengths), jnp.arange(rows * top), side="right").astype(jnp.int32)
    listing = members.reshape(top, rows).T
    listing = listing[jax.random.permutation(jax.random.fold_in(own, 1), rows)]
    rotation = jax.random.randint(jax.random.fold_in(own, 2), (rows, 1), 0, top)
    return jnp.take_along_axis(listing, (jnp.arange(top)[None, :] + rotation) % top, axis=1)


def load_shares(number_of, total, most, slope, full):
    loads = [(1 << 20) // math.isqrt(rank ** slope) + 1 for rank in range(1, number_of + 1)]
    largest = most if full else min(most, max(-(-total // number_of), total * loads[0] // sum(loads)))
    least = 1 if total - largest >= number_of - 1 else 0
    counts, rest = [largest] + [least] * (number_of - 1), total - largest - least * (number_of - 1)
    while rest > 0:
        movable = [i for i in range(1, number_of) if counts[i] < largest] or [i for i in range(1, number_of) if counts[i] < most]
        whole, left = sum([loads[i] for i in movable]), rest
        for i in movable:
            addition = min(most - counts[i], max(1, left * loads[i] // whole), rest)
            counts[i] = counts[i] + addition
            rest = rest - addition
    return np.array(counts)


def gaussian(key, shape, deviation, bound, cuts=(), held_as=jnp.bfloat16):
    drawn = deviation * jax.random.normal(key, shape, jnp.float32)
    if cuts:
        drawn = drawn * level_of(key, shape, cuts, -0.22, 0.18)
    return jnp.clip(drawn, -bound, bound).astype(held_as)


def setup_inputs(seed: int = 0) -> dict:
    seeds = jax.random.split(jax.random.key(seed), 7)
    tokens = gaussian(seeds[0], (TOKENS, D), 1.0, 6.0, ((0, 128),))
    expert_ids_keys = jax.random.split(jax.random.fold_in(seeds[1], 1), TOKENS // TOK_DEV)
    expert_ids_turns = jax.random.permutation(jax.random.fold_in(seeds[1], 3), TOKENS // TOK_DEV)
    expert_ids = jax.vmap(lambda own, number: shared_out(jax.random.fold_in(seeds[1], 2), own, number, TOK_DEV, EXPERTS, TOPK, SLOTS, 2))(expert_ids_keys, expert_ids_turns).reshape((TOKENS, TOPK))
    gate_probs = jnp.clip(0.05 + 0.45 * jax.random.uniform(seeds[2], (TOKENS, TOPK), jnp.float32) ** level_of(seeds[2], (TOKENS, TOPK), ((0, 128),), -0.2, 0.2), 0.05, 0.5)
    w_gate = gaussian(seeds[3], (EXPERTS, D, FF), D ** -0.5, 0.125, ((0, 128),))
    w_up = gaussian(seeds[4], (EXPERTS, D, FF), D ** -0.5, 0.125, ((0, 128),))
    w_down = gaussian(seeds[5], (EXPERTS, FF, D), FF ** -0.5, 0.21875, ((0, 128),))
    return dict(tokens=tokens, expert_ids=expert_ids, gate_probs=gate_probs, w_gate=w_gate, w_up=w_up, w_down=w_down)


def reference(tokens, expert_ids, gate_probs, w_gate, w_up, w_down):
    sources = N_ROW * N_COL
    flat_ids = expert_ids.reshape(sources, TOK_DEV * TOPK)
    onehot = (flat_ids[:, :, None] == jnp.arange(EXPERTS, dtype=jnp.int32)[None, None, :]).astype(jnp.int32)
    rank = jnp.sum((jnp.cumsum(onehot, axis=1) - 1) * onehot, axis=2).astype(jnp.int32)
    source = jnp.arange(sources, dtype=jnp.int32)[:, None]
    position = (flat_ids * (sources * SLOTS) + source * SLOTS + rank).reshape(-1).astype(jnp.int32)
    token_of = (jnp.arange(TOKENS * TOPK, dtype=jnp.int32) // TOPK).astype(jnp.int32)
    owner = jnp.full((EXPERTS * sources * SLOTS,), -1, jnp.int32).at[position].set(token_of)
    owner = owner.reshape(EXPERTS, sources * SLOTS)

    def one_expert(index):
        picks = owner[index]
        rows = tokens[jnp.maximum(picks, 0)]
        rows = jnp.where((picks >= 0)[:, None], rows, jnp.zeros((), tokens.dtype))
        gate = jnp.dot(rows, w_gate[index], preferred_element_type=jnp.float32)
        up = jnp.dot(rows, w_up[index], preferred_element_type=jnp.float32)
        hidden = (jax.nn.silu(gate) * up).astype(jnp.bfloat16)
        return jnp.dot(hidden, w_down[index], preferred_element_type=jnp.float32).astype(jnp.bfloat16)

    outputs = lax.map(one_expert, jnp.arange(EXPERTS, dtype=jnp.int32))
    picked = outputs.reshape(-1, D)[position].reshape(TOKENS, TOPK, D).astype(jnp.float32)
    mixed = jnp.sum(gate_probs.astype(jnp.float32)[:, :, None] * picked, axis=1)
    return mixed.astype(jnp.bfloat16)
```

```python
import functools

import jax
import jax.numpy as jnp
from jax import lax
from jax.experimental import pallas as pl
from jax.experimental.pallas import tpu as pltpu
from jax.sharding import PartitionSpec as P

MESH = pl.DeviceIdType.MESH
BF16 = jnp.bfloat16
F32 = jnp.float32
SIDE = 4
PIECES = (
    (0, 0, 384), (1, 384, 384), (2, 768, 384),
    (0, 1152, 384), (1, 1536, 256), (2, 1792, 256),
)
HALF = 1152
PLANES = ((2, 1), (2, 0), (0, 1))
ORDER = tuple((i, j) for i in range(SIDE) for j in range(SIDE) if i or j)
LINE = (1, 3, 2)
UNNAMED = -1024.0


def moe_kernel(
    slots,
    ids_in, probs_in, tok_in, wg_in, wu_in, wd_in, out_ref, *scratch,
):
    n = len(PIECES)
    tokg, scratch = scratch[:n], scratch[n:]
    xs, scratch = scratch[:n], scratch[n:]
    yr, scratch = scratch[:n], scratch[n:]
    pr, scratch = scratch[:n], scratch[n:]
    zr, scratch = scratch[:n], scratch[n:]
    (
        ids, probs, wg, wu, wd, kw_out, kw_in, kf, sel, swap, spread, xc, acc, hid, hidp,
        load_sem, k_send, k_recv, l_send, l_recv, m_send, m_recv, x_send, x_recv,
        y_send, y_recv, p_send, p_recv, z_send, z_recv,
    ) = scratch
    r = lax.axis_index("row")
    c = lax.axis_index("col")
    core = c % 2
    sign = 1 - 2 * core
    here = (r % SIDE, (c // 2) % SIDE, 2 * (r // SIDE) + c // 8)
    near = [[(h + sign * d + SIDE) % SIDE for d in range(SIDE)] for h in here]
    row_x = near[0]
    col_y = [2 * v for v in near[1]]
    row_z = [SIDE * (v // 2) for v in near[2]]
    col_z = [8 * (v % 2) for v in near[2]]
    tokens = tok_in.shape[0]
    hidden = wg.shape[1]
    group = 2 * SIDE * slots
    slab = SIDE * group
    total = SIDE * slab

    def device(d, to_core):
        return (row_z[d[2]] + row_x[d[0]], col_z[d[2]] + col_y[d[1]] + to_core)

    def remote(src, dst, send, recv, to):
        return pltpu.make_async_remote_copy(
            src_ref=src, dst_ref=dst, send_sem=send, recv_sem=recv,
            device_id=to, device_id_type=MESH,
        )

    def on_line(t, d):
        step = [0, 0, 0]
        step[t] = d
        return tuple(step)

    def in_plane(t, i, j):
        step = [0, 0, 0]
        step[PLANES[t][0]] = i
        step[PLANES[t][1]] = j
        return tuple(step)

    load_ids = pltpu.make_async_copy(ids_in, ids, load_sem.at[0])
    load_probs = pltpu.make_async_copy(probs_in, probs, load_sem.at[1])
    load_ids.start()
    load_probs.start()
    load_tok = []
    for p, (t, first, width) in enumerate(PIECES):
        copy = pltpu.make_async_copy(
            tok_in.at[:, pl.ds(first, width)], tokg[p].at[here[t], core], load_sem.at[5 + p]
        )
        copy.start()
        load_tok.append(copy)
    barrier = pltpu.get_barrier_semaphore()
    signals = 0
    for dx in range(SIDE):
        for dy in range(SIDE):
            for dz in range(SIDE):
                zeros = (dx == 0) + (dy == 0) + (dz == 0)
                if zeros in (1, 2):
                    pl.semaphore_signal(
                        barrier, inc=1, device_id=device((dx, dy, dz), core), device_id_type=MESH
                    )
                    signals += 1
                if zeros in (2, 3):
                    pl.semaphore_signal(
                        barrier, inc=1, device_id=device((dx, dy, dz), 1 - core),
                        device_id_type=MESH,
                    )
                    signals += 1

    load_ids.wait()
    load_probs.wait()
    load_w = [
        pltpu.make_async_copy(wg_in.at[0], wg, load_sem.at[2]),
        pltpu.make_async_copy(wu_in.at[0], wu, load_sem.at[3]),
        pltpu.make_async_copy(wd_in.at[0], wd, load_sem.at[4]),
    ]
    experts = ids.shape[0] * 16
    place = lax.broadcasted_iota(jnp.int32, (experts, tokens), 0)
    line_of = jnp.right_shift(place, 5)
    core_of = jnp.bitwise_and(jnp.right_shift(place, 4), 1)
    slow_of = jnp.bitwise_and(jnp.right_shift(place, 2), 3)
    fast_of = jnp.bitwise_and(place, 3)
    earlier = (
        lax.broadcasted_iota(jnp.int32, (tokens, tokens), 0)
        < lax.broadcasted_iota(jnp.int32, (tokens, tokens), 1)
    ).astype(BF16)
    for t in range(3):
        at = [None] * 3
        at[t], at[PLANES[t][0]], at[PLANES[t][1]] = line_of, slow_of, fast_of
        expert = (
            16 * (SIDE * jnp.right_shift(at[2], 1) + at[0])
            + 8 * jnp.bitwise_and(at[2], 1) + 2 * at[1] + core_of
        )
        named = jnp.zeros((experts, tokens), F32)
        weight = jnp.zeros((experts, tokens), F32)
        for k in range(ids.shape[0]):
            hit = ids[k:k + 1, :] == expert
            named = jnp.where(hit, 1.0, named)
            weight = jnp.where(hit, probs[k:k + 1, :], weight)
        rank = jnp.dot(named.astype(BF16), earlier, preferred_element_type=F32)
        key = jnp.where(named > 0.5, rank, UNNAMED).astype(BF16)
        weight = weight.astype(BF16)
        for l in range(SIDE):
            for o in range(2):
                rows = slice((2 * l + o) * 16, (2 * l + o + 1) * 16)
                kw_out[t, l, o, 0] = key[rows]
                kw_out[t, l, o, 1] = weight[rows]
        kw_in[t, 2 * here[t] + core] = kw_out[t, here[t], core]

    pl.semaphore_wait(barrier, signals)

    k_copies = []
    for t in range(3):
        for d in range(SIDE):
            for o in range(2):
                if d == 0 and o == 0:
                    continue
                to_core = core if o == 0 else 1 - core
                copy = remote(
                    kw_out.at[t, near[t][d], to_core], kw_in.at[t, 2 * here[t] + core],
                    k_send.at[t, d, o], k_recv.at[t, d, o], device(on_line(t, d), to_core),
                )
                copy.start()
                k_copies.append(copy)

    l_copies = {}
    m_copies = {}

    def to_mate(p, d):
        t = PIECES[p][0]
        block = tokg[p].at[near[t][(SIDE - d) % SIDE], core]
        copy = remote(
            block, block, m_send.at[p, d], m_recv.at[p, d], device((0, 0, 0), 1 - core)
        )
        copy.start()
        m_copies[p, d] = copy

    for p, (t, first, width) in enumerate(PIECES):
        load_tok[p].wait()
        for d in LINE:
            block = tokg[p].at[here[t], core]
            copy = remote(
                block, block, l_send.at[p, d], l_recv.at[p, d], device(on_line(t, d), core)
            )
            copy.start()
            l_copies[p, d] = copy
        to_mate(p, 0)
    for copy in load_w:
        copy.start()

    row_id = lax.broadcasted_iota(jnp.int32, (slab, slab), 0)
    col_id = lax.broadcasted_iota(jnp.int32, (slab, slab), 1)
    pair = 2 * slots
    twin = jnp.zeros((slab, slab), jnp.int32)
    for i in range(SIDE):
        for j in range(SIDE):
            first = (i * SIDE + j) * pair
            twin = jnp.where(
                (col_id >= first) & (col_id < first + pair),
                col_id + ((j * SIDE + i) * pair - first), twin,
            )
    swap[...] = (row_id == twin).astype(F32).astype(BF16)
    lane = lax.broadcasted_iota(jnp.int32, (16, total), 1)
    owner = group * lax.broadcasted_iota(jnp.int32, (16, total), 0)
    spread[...] = ((lane >= owner) & (lane < owner + group)).astype(F32).astype(BF16)

    for copy in k_copies:
        copy.wait()
    slot_of = lax.broadcasted_iota(jnp.int32, (group, tokens), 0).astype(F32)
    for t in range(3):
        def choose(s, _):
            kf[...] = kw_in[t, s, 0].astype(F32) + (s * slots).astype(F32)
            lanes = pl.ds(pl.multiple_of(s * tokens, tokens), tokens)
            for q in range(SIDE * SIDE):
                sel[t, q * group:(q + 1) * group, lanes] = (
                    slot_of == kf[q:q + 1, :]
                ).astype(F32).astype(BF16)
            return 0

        lax.fori_loop(0, 2 * SIDE, choose, 0)

    sources = 2 * SIDE * tokens
    x_copies = {}

    def forward(p):
        for d in LINE:
            l_copies[p, d].wait_recv()
            to_mate(p, d)

    def dispatch(p):
        t, first, width = PIECES[p]
        a, b = PLANES[t]
        for d in range(SIDE):
            m_copies[p, d].wait_recv()

        def select(i, _):
            rows = pl.ds(pl.multiple_of(i * slab, slab), slab)
            res = jnp.dot(
                sel[t, rows, :sources], tokg[p][...].reshape(sources, width),
                preferred_element_type=F32,
            )
            xs[p][i] = res.astype(BF16).reshape(SIDE, group, width)
            return 0

        lax.fori_loop(0, SIDE, select, 0)
        columns = pl.ds(first, width)
        for o, (i, j) in enumerate(ORDER):
            copy = remote(
                xs[p].at[near[a][i], near[b][j]], xc.at[here[a], here[b], :, columns],
                x_send.at[p, o], x_recv.at[p, o], device(in_plane(t, i, j), core),
            )
            copy.start()
            x_copies[p, o] = copy
        xc[here[a], here[b], :, columns] = xs[p][here[a], here[b]]

    for p in range(3):
        forward(p)
    for p in range(3):
        dispatch(p)
    for p in range(3, n):
        forward(p)
    for p in range(3, n):
        dispatch(p)

    lane = lax.broadcasted_iota(jnp.int32, (1, total), 1)
    slot_at = lane
    for q in range(1, SIDE * SIDE):
        slot_at = jnp.where(lane >= q * group, lane - q * group, slot_at)
    slot_at = slot_at.astype(F32)
    for t in range(3):
        def weigh(s, _):
            expand = lambda w: lax.dot_general(
                kw_in[t, s, w], spread[...], (((0,), (0,)), ((), ())),
                preferred_element_type=F32,
            )
            chosen = expand(0) + (s * slots).astype(F32) == slot_at
            value = jnp.where(chosen, expand(1), 0.0).astype(BF16)
            o, l = s // SIDE, s % SIDE
            return value

        def weigh_all(l, _):
            for o in range(2):
                rows = pl.ds(pl.multiple_of((o * SIDE + l) * tokens, tokens), tokens)
                sel[t, rows, :] = weigh(2 * l + o, 0)
            return 0

        lax.fori_loop(0, SIDE, weigh_all, 0)

    def collect(p):
        t, first, width = PIECES[p]
        for o in range(len(ORDER)):
            x_copies[p, o].wait()
        if t == 0:
            return
        columns = pl.ds(first, width)

        def reorder(i, _):
            block = xc.at[i] if t == 1 else xc.at[:, i]
            res = jnp.dot(
                swap[...], block[:, :, columns].reshape(slab, width), preferred_element_type=F32
            )
            block[:, :, columns] = res.astype(BF16).reshape(SIDE, group, width)
            return 0

        lax.fori_loop(0, SIDE, reorder, 0)

    m_rows = 2 * slab
    f_tile = 256

    def up_tiles(step):
        def one(k, _):
            for m in range(2):
                step(m, pl.multiple_of(k * f_tile, f_tile))
            return 0

        lax.fori_loop(0, hidden // f_tile, one, 0)

    def first_half(m, f):
        x = xc[2 * m:2 * m + 2, :, :, :HALF].reshape(m_rows, HALF)
        rows = slice(m * m_rows, (m + 1) * m_rows)
        acc[rows, pl.ds(f, f_tile)] = jnp.dot(
            x, wg[:HALF, pl.ds(f, f_tile)], preferred_element_type=F32
        )
        acc[rows, pl.ds(hidden + f, f_tile)] = jnp.dot(
            x, wu[:HALF, pl.ds(f, f_tile)], preferred_element_type=F32
        )

    def second_half(m, f):
        x = xc[2 * m:2 * m + 2, :, :, HALF:]
        x = x.reshape(m_rows, x.shape[-1])
        rows = slice(m * m_rows, (m + 1) * m_rows)
        gate = acc[rows, pl.ds(f, f_tile)] + jnp.dot(
            x, wg[HALF:, pl.ds(f, f_tile)], preferred_element_type=F32
        )
        up = acc[rows, pl.ds(hidden + f, f_tile)] + jnp.dot(
            x, wu[HALF:, pl.ds(f, f_tile)], preferred_element_type=F32
        )
        value = (gate / (1.0 + jnp.exp(-gate)) * up).astype(BF16)
        hid[2 * m:2 * m + 2, :, :, pl.ds(f, f_tile)] = value.reshape(2, SIDE, group, f_tile)

    for p in range(3):
        collect(p)
    for copy in load_w:
        copy.wait()
    up_tiles(first_half)
    for p in range(3, n):
        collect(p)
    up_tiles(second_half)

    def reorder_hidden(t):
        def reorder(i, _):
            src = hid.at[i] if t == 1 else hid.at[:, i]
            dst = hidp.at[t - 1, i] if t == 1 else hidp.at[t - 1, :, i]
            res = jnp.dot(
                swap[...], src[...].reshape(slab, hidden), preferred_element_type=F32
            )
            dst[...] = res.astype(BF16).reshape(SIDE, group, hidden)
            return 0

        lax.fori_loop(0, SIDE, reorder, 0)

    y_copies = {}

    def give_back(p):
        t, first, width = PIECES[p]
        a, b = PLANES[t]
        source = hid if t == 0 else hidp.at[t - 1]

        def down(i, _):
            res = jnp.dot(
                source[i].reshape(slab, hidden), wd[:, first:first + width],
                preferred_element_type=F32,
            )
            xs[p][i] = res.astype(BF16).reshape(SIDE, group, width)
            return 0

        lax.fori_loop(0, SIDE, down, 0)
        for o, (i, j) in enumerate(ORDER):
            copy = remote(
                xs[p].at[near[a][i], near[b][j]], yr[p].at[here[a], here[b]],
                y_send.at[p, o], y_recv.at[p, o], device(in_plane(t, i, j), core),
            )
            copy.start()
            y_copies[p, o] = copy
        yr[p][here[a], here[b]] = xs[p][here[a], here[b]]

    for p in range(n):
        t = PIECES[p][0]
        if p < 3 and t > 0:
            reorder_hidden(t)
        give_back(p)

    for copy in l_copies.values():
        copy.wait_send()
    for copy in m_copies.values():
        copy.wait_send()
    p_copies, z_copies = {}, {}
    half = SIDE * tokens

    def share(p):
        rows = slice(half * (p // 4), half * (p // 4 + 1))
        columns = slice(384 * (p % 4), 384 * (p % 4) + PIECES[p][2])
        return acc.at[rows, columns]

    def combine(p):
        t, first, width = PIECES[p]
        for o in range(len(ORDER)):
            y_copies[p, o].wait()

        def part(o):
            rows = pl.ds(pl.multiple_of(o * half, half), half)
            return jnp.dot(
                sel[t, rows, :], yr[p][...].reshape(total, width), preferred_element_type=F32
            )

        tokg[p][:, 0] = part(1 - core).astype(BF16).reshape(SIDE, tokens, width)
        copy = remote(
            tokg[p].at[:, 0], pr[p], p_send.at[p], p_recv.at[p], device((0, 0, 0), 1 - core)
        )
        copy.start()
        p_copies[p] = copy
        share(p)[...] = part(core)

    def reduce_cores(p):
        t, first, width = PIECES[p]
        p_copies[p].wait()
        both = share(p)[...] + pr[p][...].reshape(half, width).astype(F32)
        share(p)[...] = both
        tokg[p][:, 1] = both.astype(BF16).reshape(SIDE, tokens, width)
        for d in LINE:
            copy = remote(
                tokg[p].at[near[t][d], 1], zr[p].at[d - 1],
                z_send.at[p, d], z_recv.at[p, d], device(on_line(t, d), core),
            )
            copy.start()
            z_copies[p, d] = copy

    def finish(p):
        t, first, width = PIECES[p]
        result = share(p)[pl.ds(pl.multiple_of(here[t] * tokens, tokens), tokens), :]
        for d in LINE:
            z_copies[p, d].wait()
        for d in range(1, SIDE):
            result = result + zr[p][d - 1].astype(F32)
        out_ref[:, first:first + width] = result.astype(BF16)

    for p in range(n):
        combine(p)
        if p:
            reduce_cores(p - 1)
    reduce_cores(n - 1)
    for p in range(n):
        finish(p)


def body(tokens, expert_ids, gate_probs, w_gate, w_up, w_down):
    count, choices = expert_ids.shape
    width = tokens.shape[1]
    hidden = w_gate.shape[2]
    slots = 10
    group = 2 * SIDE * slots
    total = SIDE * SIDE * group
    n = len(PIECES)
    any_spec = pl.BlockSpec(memory_space=pl.ANY)
    dma = pltpu.SemaphoreType.DMA
    widths = [w for _, _, w in PIECES]
    scratch = (
        [pltpu.VMEM((SIDE, 2, count, w), BF16) for w in widths]
        + [pltpu.VMEM((SIDE, SIDE, group, w), BF16) for w in widths]
        + [pltpu.VMEM((SIDE, SIDE, group, w), BF16) for w in widths]
        + [pltpu.VMEM((SIDE, count, w), BF16) for w in widths]
        + [pltpu.VMEM((SIDE - 1, count, w), BF16) for w in widths]
        + [
            pltpu.VMEM((choices, count), jnp.int32),
            pltpu.VMEM((choices, count), F32),
            pltpu.VMEM((width, hidden), BF16),
            pltpu.VMEM((width, hidden), BF16),
            pltpu.VMEM((hidden, width), BF16),
            pltpu.VMEM((3, SIDE, 2, 2, 16, count), BF16),
            pltpu.VMEM((3, 2 * SIDE, 2, 16, count), BF16),
            pltpu.VMEM((16, count), F32),
            pltpu.VMEM((3, total, total), BF16),
            pltpu.VMEM((SIDE * group, SIDE * group), BF16),
            pltpu.VMEM((16, total), BF16),
            pltpu.VMEM((SIDE, SIDE, group, width), BF16),
            pltpu.VMEM((total, 2 * hidden), F32),
            pltpu.VMEM((SIDE, SIDE, group, hidden), BF16),
            pltpu.VMEM((2, SIDE, SIDE, group, hidden), BF16),
            dma((5 + n,)),
            dma((3, SIDE, 2)), dma((3, SIDE, 2)),
            dma((n, SIDE)), dma((n, SIDE)),
            dma((n, SIDE)), dma((n, SIDE)),
            dma((n, SIDE * SIDE - 1)), dma((n, SIDE * SIDE - 1)),
            dma((n, SIDE * SIDE - 1)), dma((n, SIDE * SIDE - 1)),
            dma((n,)), dma((n,)),
            dma((n, SIDE)), dma((n, SIDE)),
        ]
    )
    return pl.pallas_call(
        functools.partial(moe_kernel, slots),
        out_shape=jax.ShapeDtypeStruct((count, width), BF16),
        in_specs=[any_spec] * 6,
        out_specs=pl.BlockSpec(memory_space=pltpu.VMEM),
        scratch_shapes=scratch,
        compiler_params=pltpu.CompilerParams(
            collective_id=0, has_side_effects=True, vmem_limit_bytes=67043328
        ),
    )(expert_ids.T, gate_probs.T, tokens, w_gate, w_up, w_down)


def solution(mesh):
    in_specs = (
        P(("row", "col"), None),
        P(("row", "col"), None),
        P(("row", "col"), None),
        P(("row", "col"), None, None),
        P(("row", "col"), None, None),
        P(("row", "col"), None, None),
    )
    out_specs = P(("row", "col"), None)
    return jax.shard_map(body, mesh=mesh, in_specs=in_specs, out_specs=out_specs, check_vma=False)
```

```python
import functools

import jax
import jax.numpy as jnp
from jax import lax
from jax.experimental import pallas as pl
from jax.experimental.pallas import tpu as pltpu
from jax.sharding import PartitionSpec as P

MESH = pl.DeviceIdType.MESH
BF16 = jnp.bfloat16
F32 = jnp.float32
SIDE = 4
PIECES = (
    (0, 0, 128), (1, 128, 128), (2, 256, 128),
    (0, 384, 384), (1, 768, 256), (2, 1024, 256),
    (0, 1280, 256), (1, 1536, 256), (2, 1792, 256),
)
TRIOS = ((0, 1, 2), (3, 4, 5), (6, 7, 8))
RETURNS = (TRIOS[1], TRIOS[2], TRIOS[0])
HALF = 1280
SHARES = ((0, 896), (0, 1024), (0, 1152), (0, 0), (0, 384), (0, 640), (1, 0), (1, 256), (1, 512))
PLANES = ((2, 1), (2, 0), (0, 1))
PEERS = tuple((i, j) for i in range(SIDE) for j in range(SIDE) if i or j)
LINE = (1, 3, 2)
UNNAMED = -1024.0


def moe_kernel(
    slots,
    ids_in, probs_in, tok_in, wg_in, wu_in, wd_in, out_ref, *scratch,
):
    n = len(PIECES)
    tokg, scratch = scratch[:n], scratch[n:]
    xs, scratch = scratch[:n], scratch[n:]
    yr, scratch = scratch[:n], scratch[n:]
    pr, scratch = scratch[:n], scratch[n:]
    zr, scratch = scratch[:n], scratch[n:]
    (
        ids, probs, wg, wu, wd, kw_out, kw_in, kf, sel, swap, spread, xc, acc, hid, hidp,
        load_sem, ready, k_send, k_recv, l_send, l_recv, m_send, m_recv, x_send, x_recv,
        y_send, y_recv, p_send, p_recv, z_send, z_recv,
    ) = scratch
    r = lax.axis_index("row")
    c = lax.axis_index("col")
    core = c % 2
    sign = 1 - 2 * core
    here = (r % SIDE, (c // 2) % SIDE, 2 * (r // SIDE) + c // 8)
    near = [[(h + sign * d + SIDE) % SIDE for d in range(SIDE)] for h in here]
    row_x = near[0]
    col_y = [2 * v for v in near[1]]
    row_z = [SIDE * (v // 2) for v in near[2]]
    col_z = [8 * (v % 2) for v in near[2]]
    tokens = tok_in.shape[0]
    hidden = wg.shape[1]
    group = 2 * SIDE * slots
    slab = SIDE * group
    total = SIDE * slab

    def device(d, to_core):
        return (row_z[d[2]] + row_x[d[0]], col_z[d[2]] + col_y[d[1]] + to_core)

    def remote(src, dst, send, recv, to):
        return pltpu.make_async_remote_copy(
            src_ref=src, dst_ref=dst, send_sem=send, recv_sem=recv,
            device_id=to, device_id_type=MESH,
        )

    def on_line(t, d):
        step = [0, 0, 0]
        step[t] = d
        return tuple(step)

    def in_plane(t, i, j):
        step = [0, 0, 0]
        step[PLANES[t][0]] = i
        step[PLANES[t][1]] = j
        return tuple(step)

    load_ids = pltpu.make_async_copy(ids_in, ids, load_sem.at[0])
    load_probs = pltpu.make_async_copy(probs_in, probs, load_sem.at[1])
    load_ids.start()
    load_probs.start()
    load_tok = []
    for p, (t, first, width) in enumerate(PIECES):
        copy = pltpu.make_async_copy(
            tok_in.at[:, pl.ds(first, width)], tokg[p].at[here[t], core], load_sem.at[5 + p]
        )
        copy.start()
        load_tok.append(copy)
    barrier = pltpu.get_barrier_semaphore()

    def greet(semaphore, to):
        pl.semaphore_signal(semaphore, inc=1, device_id=to, device_id_type=MESH)

    greet(barrier, device((0, 0, 0), 1 - core))
    for d in LINE:
        for t in range(3):
            greet(barrier, device(on_line(t, d), core))

    load_ids.wait()
    load_probs.wait()
    load_w = [
        pltpu.make_async_copy(wg_in.at[0], wg, load_sem.at[2]),
        pltpu.make_async_copy(wu_in.at[0], wu, load_sem.at[3]),
        pltpu.make_async_copy(wd_in.at[0], wd, load_sem.at[4]),
    ]
    experts = ids.shape[0] * 16
    place = lax.broadcasted_iota(jnp.int32, (experts, tokens), 0)
    line_of = jnp.right_shift(place, 5)
    core_of = jnp.bitwise_and(jnp.right_shift(place, 4), 1)
    slow_of = jnp.bitwise_and(jnp.right_shift(place, 2), 3)
    fast_of = jnp.bitwise_and(place, 3)
    earlier = (
        lax.broadcasted_iota(jnp.int32, (tokens, tokens), 0)
        < lax.broadcasted_iota(jnp.int32, (tokens, tokens), 1)
    ).astype(BF16)
    for t in range(3):
        at = [None] * 3
        at[t], at[PLANES[t][0]], at[PLANES[t][1]] = line_of, slow_of, fast_of
        expert = (
            16 * (SIDE * jnp.right_shift(at[2], 1) + at[0])
            + 8 * jnp.bitwise_and(at[2], 1) + 2 * at[1] + core_of
        )
        named = jnp.zeros((experts, tokens), F32)
        weight = jnp.zeros((experts, tokens), F32)
        for k in range(ids.shape[0]):
            hit = ids[k:k + 1, :] == expert
            named = jnp.where(hit, 1.0, named)
            weight = jnp.where(hit, probs[k:k + 1, :], weight)
        rank = jnp.dot(named.astype(BF16), earlier, preferred_element_type=F32)
        key = jnp.where(named > 0.5, rank, UNNAMED).astype(BF16)
        weight = weight.astype(BF16)
        for l in range(SIDE):
            for o in range(2):
                rows = slice((2 * l + o) * 16, (2 * l + o + 1) * 16)
                kw_out[t, l, o, 0] = key[rows]
                kw_out[t, l, o, 1] = weight[rows]
        kw_in[t, 2 * here[t] + core] = kw_out[t, here[t], core]

    pl.semaphore_wait(barrier, 1 + 3 * len(LINE))
    greet(ready.at[0], device((0, 0, 0), 1 - core))
    for d in LINE:
        for t in range(3):
            greet(ready.at[1], device(on_line(t, d), core))

    k_copies = []

    def send_keys(t, d, o):
        to_core = core if o == 0 else 1 - core
        copy = remote(
            kw_out.at[t, near[t][d], to_core], kw_in.at[t, 2 * here[t] + core],
            k_send.at[t, d, o], k_recv.at[t, d, o], device(on_line(t, d), to_core),
        )
        copy.start()
        k_copies.append(copy)

    l_copies = {}
    m_copies = {}

    def to_mate(p, d):
        t = PIECES[p][0]
        block = tokg[p].at[near[t][(SIDE - d) % SIDE], core]
        copy = remote(
            block, block, m_send.at[p, d], m_recv.at[p, d], device((0, 0, 0), 1 - core)
        )
        copy.start()
        m_copies[p, d] = copy

    def send_tokens(trio):
        for p in trio:
            load_tok[p].wait()
        for d in LINE:
            for p in trio:
                t = PIECES[p][0]
                block = tokg[p].at[here[t], core]
                copy = remote(
                    block, block, l_send.at[p, d], l_recv.at[p, d], device(on_line(t, d), core)
                )
                copy.start()
                l_copies[p, d] = copy
        for p in trio:
            to_mate(p, 0)

    send_tokens(TRIOS[0])
    for t in range(3):
        for d in LINE:
            send_keys(t, d, 0)
        send_keys(t, 0, 1)
    pl.semaphore_wait(ready.at[0], 1)
    for t in range(3):
        for d in LINE:
            send_keys(t, d, 1)
    for trio in TRIOS[1:]:
        send_tokens(trio)
    for copy in load_w:
        copy.start()

    row_id = lax.broadcasted_iota(jnp.int32, (slab, slab), 0)
    col_id = lax.broadcasted_iota(jnp.int32, (slab, slab), 1)
    pair = 2 * slots
    twin = jnp.zeros((slab, slab), jnp.int32)
    for i in range(SIDE):
        for j in range(SIDE):
            first = (i * SIDE + j) * pair
            twin = jnp.where(
                (col_id >= first) & (col_id < first + pair),
                col_id + ((j * SIDE + i) * pair - first), twin,
            )
    swap[...] = (row_id == twin).astype(F32).astype(BF16)
    lane = lax.broadcasted_iota(jnp.int32, (16, total), 1)
    owner = group * lax.broadcasted_iota(jnp.int32, (16, total), 0)
    spread[...] = ((lane >= owner) & (lane < owner + group)).astype(F32).astype(BF16)

    for copy in k_copies:
        copy.wait()
    slot_of = lax.broadcasted_iota(jnp.int32, (group, tokens), 0).astype(F32)
    for t in range(3):
        def choose(s, _):
            kf[...] = kw_in[t, s, 0].astype(F32) + (s * slots).astype(F32)
            lanes = pl.ds(pl.multiple_of(s * tokens, tokens), tokens)
            for q in range(SIDE * SIDE):
                sel[t, q * group:(q + 1) * group, lanes] = (
                    slot_of == kf[q:q + 1, :]
                ).astype(F32).astype(BF16)
            return 0

        lax.fori_loop(0, 2 * SIDE, choose, 0)

    def exchange(trio, product, landing, send, recv):
        copies = {}

        def peer(p, i, j, v):
            a, b = PLANES[PIECES[p][0]]
            at = list(here)
            at[a], at[b] = v, near[b][j]
            return remote(
                xs[p].at[v, near[b][j]], landing(p, here[a], here[b]),
                send.at[p, i, j], recv.at[p, i, j],
                (SIDE * (at[2] // 2) + at[0], 8 * (at[2] % 2) + 2 * at[1] + core),
            )

        def slab_of(i, _):
            where = []
            for p in trio:
                v = (here[PLANES[PIECES[p][0]][0]] + sign * i + SIDE) % SIDE
                xs[p][v] = product(p, v).astype(BF16).reshape(SIDE, group, PIECES[p][2])
                where.append(v)

            @pl.when(i > 0)
            def _():
                for p, v in zip(trio, where):
                    peer(p, i, 0, v).start()

            for j in range(1, SIDE):
                for p, v in zip(trio, where):
                    peer(p, i, j, v).start()
            return 0

        lax.fori_loop(0, SIDE, slab_of, 0)
        for p in trio:
            a, b = PLANES[PIECES[p][0]]
            landing(p, here[a], here[b])[...] = xs[p][here[a], here[b]]
            for i, j in PEERS:
                copies[p, i, j] = peer(p, i, j, near[a][i])
        return copies

    sources = 2 * SIDE * tokens
    x_copies = {}

    def forward(p):
        for d in LINE:
            l_copies[p, d].wait_recv()
            to_mate(p, d)

    def select(p, v):
        t, first, width = PIECES[p]
        rows = pl.ds(pl.multiple_of(v * slab, slab), slab)
        return jnp.dot(
            sel[t, rows, :sources], tokg[p][...].reshape(sources, width),
            preferred_element_type=F32,
        )

    def arrival(p, u, v):
        return xc.at[u, v, :, pl.ds(PIECES[p][1], PIECES[p][2])]

    for p in TRIOS[0]:
        forward(p)
    for trio in TRIOS:
        for p in trio:
            for d in range(SIDE):
                m_copies[p, d].wait_recv()
        if trio == TRIOS[0]:
            pl.semaphore_wait(ready.at[1], 3 * len(LINE))
        x_copies.update(exchange(trio, select, arrival, x_send, x_recv))
        if trio != TRIOS[-1]:
            for p in TRIOS[TRIOS.index(trio) + 1]:
                forward(p)

    lane = lax.broadcasted_iota(jnp.int32, (1, total), 1)
    slot_at = lane
    for q in range(1, SIDE * SIDE):
        slot_at = jnp.where(lane >= q * group, lane - q * group, slot_at)
    slot_at = slot_at.astype(F32)
    for t in range(3):
        def weigh(s, _):
            expand = lambda w: lax.dot_general(
                kw_in[t, s, w], spread[...], (((0,), (0,)), ((), ())),
                preferred_element_type=F32,
            )
            chosen = expand(0) + (s * slots).astype(F32) == slot_at
            value = jnp.where(chosen, expand(1), 0.0).astype(BF16)
            o, l = s // SIDE, s % SIDE
            return value

        def weigh_all(l, _):
            for o in range(2):
                rows = pl.ds(pl.multiple_of((o * SIDE + l) * tokens, tokens), tokens)
                sel[t, rows, :] = weigh(2 * l + o, 0)
            return 0

        lax.fori_loop(0, SIDE, weigh_all, 0)

    def collect(p):
        t, first, width = PIECES[p]
        for i, j in PEERS:
            x_copies[p, i, j].wait()
        if t == 0:
            return
        columns = pl.ds(first, width)

        def reorder(i, _):
            block = xc.at[i] if t == 1 else xc.at[:, i]
            res = jnp.dot(
                swap[...], block[:, :, columns].reshape(slab, width), preferred_element_type=F32
            )
            block[:, :, columns] = res.astype(BF16).reshape(SIDE, group, width)
            return 0

        lax.fori_loop(0, SIDE, reorder, 0)

    m_rows = 2 * slab
    f_tile = 256

    def up_tiles(step):
        def one(k, _):
            for m in range(2):
                step(m, pl.multiple_of(k * f_tile, f_tile))
            return 0

        lax.fori_loop(0, hidden // f_tile, one, 0)

    def first_half(m, f):
        x = xc[2 * m:2 * m + 2, :, :, :HALF].reshape(m_rows, HALF)
        rows = slice(m * m_rows, (m + 1) * m_rows)
        acc[rows, pl.ds(f, f_tile)] = jnp.dot(
            x, wg[:HALF, pl.ds(f, f_tile)], preferred_element_type=F32
        )
        acc[rows, pl.ds(hidden + f, f_tile)] = jnp.dot(
            x, wu[:HALF, pl.ds(f, f_tile)], preferred_element_type=F32
        )

    def second_half(m, f):
        x = xc[2 * m:2 * m + 2, :, :, HALF:]
        x = x.reshape(m_rows, x.shape[-1])
        rows = slice(m * m_rows, (m + 1) * m_rows)
        gate = acc[rows, pl.ds(f, f_tile)] + jnp.dot(
            x, wg[HALF:, pl.ds(f, f_tile)], preferred_element_type=F32
        )
        up = acc[rows, pl.ds(hidden + f, f_tile)] + jnp.dot(
            x, wu[HALF:, pl.ds(f, f_tile)], preferred_element_type=F32
        )
        value = (gate / (1.0 + jnp.exp(-gate)) * up).astype(BF16)
        hid[2 * m:2 * m + 2, :, :, pl.ds(f, f_tile)] = value.reshape(2, SIDE, group, f_tile)

    for p in TRIOS[0] + TRIOS[1]:
        collect(p)
    for copy in load_w:
        copy.wait()
    up_tiles(first_half)
    for p in TRIOS[2]:
        collect(p)
    up_tiles(second_half)

    def reorder_hidden(t):
        def reorder(i, _):
            src = hid.at[i] if t == 1 else hid.at[:, i]
            dst = hidp.at[t - 1, i] if t == 1 else hidp.at[t - 1, :, i]
            res = jnp.dot(
                swap[...], src[...].reshape(slab, hidden), preferred_element_type=F32
            )
            dst[...] = res.astype(BF16).reshape(SIDE, group, hidden)
            return 0

        lax.fori_loop(0, SIDE, reorder, 0)

    y_copies = {}

    def down(p, v):
        t, first, width = PIECES[p]
        source = hid if t == 0 else hidp.at[t - 1]
        return jnp.dot(
            source[v].reshape(slab, hidden), wd[:, first:first + width],
            preferred_element_type=F32,
        )

    for t in (1, 2):
        reorder_hidden(t)
    for trio in RETURNS:
        y_copies.update(exchange(trio, down, lambda p, u, v: yr[p].at[u, v], y_send, y_recv))

    for copy in l_copies.values():
        copy.wait_send()
    for copy in m_copies.values():
        copy.wait_send()
    p_copies, z_copies = {}, {}
    half = SIDE * tokens

    def share(p):
        band, first = SHARES[p]
        return acc.at[half * band:half * (band + 1), first:first + PIECES[p][2]]

    def combine(p):
        t, first, width = PIECES[p]
        for i, j in PEERS:
            y_copies[p, i, j].wait()

        def part(o):
            rows = pl.ds(pl.multiple_of(o * half, half), half)
            return jnp.dot(
                sel[t, rows, :], yr[p][...].reshape(total, width), preferred_element_type=F32
            )

        tokg[p][:, 0] = part(1 - core).astype(BF16).reshape(SIDE, tokens, width)
        copy = remote(
            tokg[p].at[:, 0], pr[p], p_send.at[p], p_recv.at[p], device((0, 0, 0), 1 - core)
        )
        copy.start()
        p_copies[p] = copy
        share(p)[...] = part(core)

    def reduce_cores(p):
        t, first, width = PIECES[p]
        p_copies[p].wait()
        both = share(p)[...] + pr[p][...].reshape(half, width).astype(F32)
        share(p)[...] = both
        tokg[p][:, 1] = both.astype(BF16).reshape(SIDE, tokens, width)
        for d in LINE:
            copy = remote(
                tokg[p].at[near[t][d], 1], zr[p].at[d - 1],
                z_send.at[p, d], z_recv.at[p, d], device(on_line(t, d), core),
            )
            copy.start()
            z_copies[p, d] = copy

    def finish(p):
        t, first, width = PIECES[p]
        result = share(p)[pl.ds(pl.multiple_of(here[t] * tokens, tokens), tokens), :]
        for d in LINE:
            z_copies[p, d].wait()
        for d in range(1, SIDE):
            result = result + zr[p][d - 1].astype(F32)
        out_ref[:, first:first + width] = result.astype(BF16)

    for trio in RETURNS:
        for p in trio:
            combine(p)
        if trio != RETURNS[0]:
            for p in RETURNS[RETURNS.index(trio) - 1]:
                finish(p)
        for p in trio:
            reduce_cores(p)
    for p in RETURNS[-1]:
        finish(p)


def body(tokens, expert_ids, gate_probs, w_gate, w_up, w_down):
    count, choices = expert_ids.shape
    width = tokens.shape[1]
    hidden = w_gate.shape[2]
    slots = 10
    group = 2 * SIDE * slots
    total = SIDE * SIDE * group
    n = len(PIECES)
    any_spec = pl.BlockSpec(memory_space=pl.ANY)
    dma = pltpu.SemaphoreType.DMA
    widths = [w for _, _, w in PIECES]
    scratch = (
        [pltpu.VMEM((SIDE, 2, count, w), BF16) for w in widths]
        + [pltpu.VMEM((SIDE, SIDE, group, w), BF16) for w in widths]
        + [pltpu.VMEM((SIDE, SIDE, group, w), BF16) for w in widths]
        + [pltpu.VMEM((SIDE, count, w), BF16) for w in widths]
        + [pltpu.VMEM((SIDE - 1, count, w), BF16) for w in widths]
        + [
            pltpu.VMEM((choices, count), jnp.int32),
            pltpu.VMEM((choices, count), F32),
            pltpu.VMEM((width, hidden), BF16),
            pltpu.VMEM((width, hidden), BF16),
            pltpu.VMEM((hidden, width), BF16),
            pltpu.VMEM((3, SIDE, 2, 2, 16, count), BF16),
            pltpu.VMEM((3, 2 * SIDE, 2, 16, count), BF16),
            pltpu.VMEM((16, count), F32),
            pltpu.VMEM((3, total, total), BF16),
            pltpu.VMEM((SIDE * group, SIDE * group), BF16),
            pltpu.VMEM((16, total), BF16),
            pltpu.VMEM((SIDE, SIDE, group, width), BF16),
            pltpu.VMEM((total, 2 * hidden), F32),
            pltpu.VMEM((SIDE, SIDE, group, hidden), BF16),
            pltpu.VMEM((2, SIDE, SIDE, group, hidden), BF16),
            dma((5 + n,)),
            pltpu.SemaphoreType.REGULAR((2,)),
            dma((3, SIDE, 2)), dma((3, SIDE, 2)),
            dma((n, SIDE)), dma((n, SIDE)),
            dma((n, SIDE)), dma((n, SIDE)),
            dma((n, SIDE, SIDE)), dma((n, SIDE, SIDE)),
            dma((n, SIDE, SIDE)), dma((n, SIDE, SIDE)),
            dma((n,)), dma((n,)),
            dma((n, SIDE)), dma((n, SIDE)),
        ]
    )
    return pl.pallas_call(
        functools.partial(moe_kernel, slots),
        out_shape=jax.ShapeDtypeStruct((count, width), BF16),
        in_specs=[any_spec] * 6,
        out_specs=pl.BlockSpec(memory_space=pltpu.VMEM),
        scratch_shapes=scratch,
        compiler_params=pltpu.CompilerParams(
            collective_id=0, has_side_effects=True, vmem_limit_bytes=67043328
        ),
    )(expert_ids.T, gate_probs.T, tokens, w_gate, w_up, w_down)


def solution(mesh):
    in_specs = (
        P(("row", "col"), None),
        P(("row", "col"), None),
        P(("row", "col"), None),
        P(("row", "col"), None, None),
        P(("row", "col"), None, None),
        P(("row", "col"), None, None),
    )
    out_specs = P(("row", "col"), None)
    return jax.shard_map(body, mesh=mesh, in_specs=in_specs, out_specs=out_specs, check_vma=False)
```

```python
import functools

import jax
import jax.numpy as jnp
from jax import lax
from jax.experimental import pallas as pl
from jax.experimental.pallas import tpu as pltpu
from jax.sharding import PartitionSpec as P

MESH = pl.DeviceIdType.MESH
BF16 = jnp.bfloat16
F32 = jnp.float32
SIDE = 4
PIECES = (
    (0, 0, 128), (1, 128, 128), (2, 256, 128),
    (0, 384, 384), (1, 768, 256), (2, 1024, 256),
    (0, 1280, 256), (1, 1536, 256), (2, 1792, 256),
)
TRIOS = ((0, 1, 2), (3, 4, 5), (6, 7, 8))
RETURNS = (TRIOS[1], TRIOS[2], TRIOS[0])
HALF = 1280
SHARES = ((0, 896), (0, 1024), (0, 1152), (0, 0), (0, 384), (0, 640), (1, 0), (1, 256), (1, 512))
PLANES = ((2, 1), (2, 0), (0, 1))
PEERS = tuple((i, j) for i in range(SIDE) for j in range(SIDE) if i or j)
LINE = (1, 3, 2)
UNNAMED = -1024.0


def moe_kernel(
    slots,
    ids_in, probs_in, tok_in, wg_in, wu_in, wd_in, out_ref, *scratch,
):
    n = len(PIECES)
    tokg, scratch = scratch[:n], scratch[n:]
    xs, scratch = scratch[:n], scratch[n:]
    yr, scratch = scratch[:n], scratch[n:]
    pr, scratch = scratch[:n], scratch[n:]
    zr, scratch = scratch[:n], scratch[n:]
    (
        ids, probs, wg, wu, wd, kw_out, kw_in, kf, sel, swap, spread, xc, acc, hid, hidp,
        load_sem, ready, k_send, k_recv, l_send, l_recv, m_send, m_recv, x_send, x_recv,
        y_send, y_recv, p_send, p_recv, z_send, z_recv,
    ) = scratch
    r = lax.axis_index("row")
    c = lax.axis_index("col")
    core = c % 2
    sign = 1 - 2 * core
    here = (r % SIDE, (c // 2) % SIDE, 2 * (r // SIDE) + c // 8)
    near = [[(h + sign * d + SIDE) % SIDE for d in range(SIDE)] for h in here]
    row_x = near[0]
    col_y = [2 * v for v in near[1]]
    row_z = [SIDE * (v // 2) for v in near[2]]
    col_z = [8 * (v % 2) for v in near[2]]
    tokens = tok_in.shape[0]
    hidden = wg.shape[1]
    group = 2 * SIDE * slots
    slab = SIDE * group
    total = SIDE * slab

    def device(d, to_core):
        return (row_z[d[2]] + row_x[d[0]], col_z[d[2]] + col_y[d[1]] + to_core)

    def remote(src, dst, send, recv, to):
        return pltpu.make_async_remote_copy(
            src_ref=src, dst_ref=dst, send_sem=send, recv_sem=recv,
            device_id=to, device_id_type=MESH,
        )

    def on_line(t, d):
        step = [0, 0, 0]
        step[t] = d
        return tuple(step)

    def in_plane(t, i, j):
        step = [0, 0, 0]
        step[PLANES[t][0]] = i
        step[PLANES[t][1]] = j
        return tuple(step)

    load_ids = pltpu.make_async_copy(ids_in, ids, load_sem.at[0])
    load_probs = pltpu.make_async_copy(probs_in, probs, load_sem.at[1])
    load_ids.start()
    load_probs.start()
    load_tok = []
    for p, (t, first, width) in enumerate(PIECES):
        copy = pltpu.make_async_copy(
            tok_in.at[:, pl.ds(first, width)], tokg[p].at[here[t], core], load_sem.at[5 + p]
        )
        copy.start()
        load_tok.append(copy)
    barrier = pltpu.get_barrier_semaphore()

    def greet(semaphore, to):
        pl.semaphore_signal(semaphore, inc=1, device_id=to, device_id_type=MESH)

    greet(barrier, device((0, 0, 0), 1 - core))
    for d in LINE:
        for t in range(3):
            greet(barrier, device(on_line(t, d), core))

    load_ids.wait()
    load_probs.wait()
    load_w = [
        pltpu.make_async_copy(wg_in.at[0], wg, load_sem.at[2]),
        pltpu.make_async_copy(wu_in.at[0], wu, load_sem.at[3]),
        pltpu.make_async_copy(wd_in.at[0], wd, load_sem.at[4]),
    ]
    experts = ids.shape[0] * 16
    place = lax.broadcasted_iota(jnp.int32, (experts, tokens), 0)
    line_of = jnp.right_shift(place, 5)
    core_of = jnp.bitwise_and(jnp.right_shift(place, 4), 1)
    slow_of = jnp.bitwise_and(jnp.right_shift(place, 2), 3)
    fast_of = jnp.bitwise_and(place, 3)
    earlier = (
        lax.broadcasted_iota(jnp.int32, (tokens, tokens), 0)
        < lax.broadcasted_iota(jnp.int32, (tokens, tokens), 1)
    ).astype(BF16)
    for t in range(3):
        at = [None] * 3
        at[t], at[PLANES[t][0]], at[PLANES[t][1]] = line_of, slow_of, fast_of
        expert = (
            16 * (SIDE * jnp.right_shift(at[2], 1) + at[0])
            + 8 * jnp.bitwise_and(at[2], 1) + 2 * at[1] + core_of
        )
        named = jnp.zeros((experts, tokens), F32)
        weight = jnp.zeros((experts, tokens), F32)
        for k in range(ids.shape[0]):
            hit = ids[k:k + 1, :] == expert
            named = jnp.where(hit, 1.0, named)
            weight = jnp.where(hit, probs[k:k + 1, :], weight)
        rank = jnp.dot(named.astype(BF16), earlier, preferred_element_type=F32)
        key = jnp.where(named > 0.5, rank, UNNAMED).astype(BF16)
        weight = weight.astype(BF16)
        for l in range(SIDE):
            for o in range(2):
                rows = slice((2 * l + o) * 16, (2 * l + o + 1) * 16)
                kw_out[t, l, o, 0] = key[rows]
                kw_out[t, l, o, 1] = weight[rows]
        kw_in[t, 2 * here[t] + core] = kw_out[t, here[t], core]

    pl.semaphore_wait(barrier, 1 + 3 * len(LINE))
    greet(ready.at[0], device((0, 0, 0), 1 - core))
    for d in LINE:
        for t in range(3):
            greet(ready.at[1], device(on_line(t, d), core))

    k_copies = {}

    def send_keys(t, d, o):
        to_core = core if o == 0 else 1 - core
        copy = remote(
            kw_out.at[t, near[t][d], to_core], kw_in.at[t, 2 * here[t] + core],
            k_send.at[t, d, o], k_recv.at[t, d, o], device(on_line(t, d), to_core),
        )
        copy.start()
        k_copies[t, d, o] = copy

    l_copies = {}
    m_copies = {}

    def to_mate(p, d):
        t = PIECES[p][0]
        block = tokg[p].at[near[t][(SIDE - d) % SIDE], core]
        copy = remote(
            block, block, m_send.at[p, d], m_recv.at[p, d], device((0, 0, 0), 1 - core)
        )
        copy.start()
        m_copies[p, d] = copy

    def send_tokens(trio):
        for p in trio:
            load_tok[p].wait()
        for d in LINE:
            for p in trio:
                t = PIECES[p][0]
                block = tokg[p].at[here[t], core]
                copy = remote(
                    block, block, l_send.at[p, d], l_recv.at[p, d], device(on_line(t, d), core)
                )
                copy.start()
                l_copies[p, d] = copy
        for p in trio:
            to_mate(p, 0)

    for t in range(3):
        for d in LINE:
            send_keys(t, d, 0)
        send_keys(t, 0, 1)
    send_tokens(TRIOS[0])
    pl.semaphore_wait(ready.at[0], 1)
    for t in range(3):
        for d in LINE:
            send_keys(t, d, 1)
    for trio in TRIOS[1:]:
        send_tokens(trio)
    for copy in load_w:
        copy.start()

    row_id = lax.broadcasted_iota(jnp.int32, (slab, slab), 0)
    col_id = lax.broadcasted_iota(jnp.int32, (slab, slab), 1)
    pair = 2 * slots
    twin = jnp.zeros((slab, slab), jnp.int32)
    for i in range(SIDE):
        for j in range(SIDE):
            first = (i * SIDE + j) * pair
            twin = jnp.where(
                (col_id >= first) & (col_id < first + pair),
                col_id + ((j * SIDE + i) * pair - first), twin,
            )
    swap[...] = (row_id == twin).astype(F32).astype(BF16)
    lane = lax.broadcasted_iota(jnp.int32, (16, total), 1)
    owner = group * lax.broadcasted_iota(jnp.int32, (16, total), 0)
    spread[...] = ((lane >= owner) & (lane < owner + group)).astype(F32).astype(BF16)

    def forward(p):
        for d in LINE:
            l_copies[p, d].wait_recv()
            to_mate(p, d)

    slot_of = lax.broadcasted_iota(jnp.int32, (group, tokens), 0).astype(F32)
    for t in range(3):
        def choose(s, _):
            kf[...] = kw_in[t, s, 0].astype(F32) + (s * slots).astype(F32)
            lanes = pl.ds(pl.multiple_of(s * tokens, tokens), tokens)
            for q in range(SIDE * SIDE):
                sel[t, q * group:(q + 1) * group, lanes] = (
                    slot_of == kf[q:q + 1, :]
                ).astype(F32).astype(BF16)
            return 0

        for (kind, d, o), copy in k_copies.items():
            if kind == t:
                copy.wait()
        lax.fori_loop(0, 2 * SIDE, choose, 0)
        if t == 0:
            for p in TRIOS[0]:
                forward(p)

    def exchange(trio, product, landing, send, recv, prepare=None):
        copies = {}

        def peer(p, i, j, v):
            a, b = PLANES[PIECES[p][0]]
            at = list(here)
            at[a], at[b] = v, near[b][j]
            return remote(
                xs[p].at[v, near[b][j]], landing(p, here[a], here[b]),
                send.at[p, i, j], recv.at[p, i, j],
                (SIDE * (at[2] // 2) + at[0], 8 * (at[2] % 2) + 2 * at[1] + core),
            )

        def slab_of(i, _):
            where = []
            if prepare is not None:
                prepare((here[PLANES[PIECES[trio[0]][0]][0]] + sign * i + SIDE) % SIDE)
            for p in trio:
                v = (here[PLANES[PIECES[p][0]][0]] + sign * i + SIDE) % SIDE
                xs[p][v] = product(p, v).astype(BF16).reshape(SIDE, group, PIECES[p][2])
                where.append(v)

            @pl.when(i > 0)
            def _():
                for p, v in zip(trio, where):
                    peer(p, i, 0, v).start()

            for j in range(1, SIDE):
                for p, v in zip(trio, where):
                    peer(p, i, j, v).start()
            return 0

        lax.fori_loop(0, SIDE, slab_of, 0)
        for p in trio:
            a, b = PLANES[PIECES[p][0]]
            landing(p, here[a], here[b])[...] = xs[p][here[a], here[b]]
            for i, j in PEERS:
                copies[p, i, j] = peer(p, i, j, near[a][i])
        return copies

    sources = 2 * SIDE * tokens
    x_copies = {}

    def select(p, v):
        t, first, width = PIECES[p]
        rows = pl.ds(pl.multiple_of(v * slab, slab), slab)
        return jnp.dot(
            sel[t, rows, :sources], tokg[p][...].reshape(sources, width),
            preferred_element_type=F32,
        )

    def arrival(p, u, v):
        return xc.at[u, v, :, pl.ds(PIECES[p][1], PIECES[p][2])]

    for trio in TRIOS:
        for p in trio:
            for d in range(SIDE):
                m_copies[p, d].wait_recv()
        if trio == TRIOS[0]:
            pl.semaphore_wait(ready.at[1], 3 * len(LINE))
        x_copies.update(exchange(trio, select, arrival, x_send, x_recv))
        if trio != TRIOS[-1]:
            for p in TRIOS[TRIOS.index(trio) + 1]:
                forward(p)

    lane = lax.broadcasted_iota(jnp.int32, (1, total), 1)
    slot_at = lane
    for q in range(1, SIDE * SIDE):
        slot_at = jnp.where(lane >= q * group, lane - q * group, slot_at)
    slot_at = slot_at.astype(F32)
    for t in range(3):
        def weigh(s, _):
            expand = lambda w: lax.dot_general(
                kw_in[t, s, w], spread[...], (((0,), (0,)), ((), ())),
                preferred_element_type=F32,
            )
            chosen = expand(0) + (s * slots).astype(F32) == slot_at
            value = jnp.where(chosen, expand(1), 0.0).astype(BF16)
            o, l = s // SIDE, s % SIDE
            return value

        def weigh_all(l, _):
            for o in range(2):
                rows = pl.ds(pl.multiple_of((o * SIDE + l) * tokens, tokens), tokens)
                sel[t, rows, :] = weigh(2 * l + o, 0)
            return 0

        lax.fori_loop(0, SIDE, weigh_all, 0)

    def arrive(p):
        for i, j in PEERS:
            x_copies[p, i, j].wait()

    def reorder(p, i):
        t, first, width = PIECES[p]
        block = xc.at[i] if t == 1 else xc.at[:, i]
        columns = pl.ds(first, width)
        res = jnp.dot(
            swap[...], block[:, :, columns].reshape(slab, width), preferred_element_type=F32
        )
        block[:, :, columns] = res.astype(BF16).reshape(SIDE, group, width)

    def reorder_all(p):
        def one(i, _):
            reorder(p, i)
            return 0

        lax.fori_loop(0, SIDE, one, 0)

    f_tile = 256
    m_rows = 2 * slab

    def first_half(k, _):
        f = pl.multiple_of(k * f_tile, f_tile)
        for m in range(2):
            x = xc[2 * m:2 * m + 2, :, :, :HALF].reshape(m_rows, HALF)
            rows = slice(m * m_rows, (m + 1) * m_rows)
            acc[rows, pl.ds(f, f_tile)] = jnp.dot(
                x, wg[:HALF, pl.ds(f, f_tile)], preferred_element_type=F32
            )
            acc[rows, pl.ds(hidden + f, f_tile)] = jnp.dot(
                x, wu[:HALF, pl.ds(f, f_tile)], preferred_element_type=F32
            )
        return 0

    def reorder_hidden(t, i):
        src = hid.at[i] if t == 1 else hid.at[:, i]
        dst = hidp.at[t - 1, i] if t == 1 else hidp.at[t - 1, :, i]
        res = jnp.dot(swap[...], src[...].reshape(slab, hidden), preferred_element_type=F32)
        dst[...] = res.astype(BF16).reshape(SIDE, group, hidden)

    def second_half(v):
        reorder(TRIOS[2][1], v)
        rows = pl.ds(pl.multiple_of(v * slab, slab), slab)

        def one(k, _):
            f = pl.multiple_of(k * f_tile, f_tile)
            x = xc[v, :, :, HALF:]
            x = x.reshape(slab, x.shape[-1])
            gate = acc[rows, pl.ds(f, f_tile)] + jnp.dot(
                x, wg[HALF:, pl.ds(f, f_tile)], preferred_element_type=F32
            )
            up = acc[rows, pl.ds(hidden + f, f_tile)] + jnp.dot(
                x, wu[HALF:, pl.ds(f, f_tile)], preferred_element_type=F32
            )
            value = (gate / (1.0 + jnp.exp(-gate)) * up).astype(BF16)
            hid[v, :, :, pl.ds(f, f_tile)] = value.reshape(SIDE, group, f_tile)
            return 0

        lax.fori_loop(0, hidden // f_tile, one, 0)
        reorder_hidden(1, v)

    for p in TRIOS[0] + TRIOS[1]:
        arrive(p)
        if PIECES[p][0] > 0:
            reorder_all(p)
    for copy in load_w:
        copy.wait()
    lax.fori_loop(0, hidden // f_tile, first_half, 0)
    for p in TRIOS[2]:
        arrive(p)
    reorder_all(TRIOS[2][2])

    y_copies = {}

    def down(p, v):
        t, first, width = PIECES[p]
        source = hid if t == 0 else hidp.at[t - 1]
        return jnp.dot(
            source[v].reshape(slab, hidden), wd[:, first:first + width],
            preferred_element_type=F32,
        )

    def reorder_last(i, _):
        reorder_hidden(2, i)
        return 0

    def give_back(trio, prepare=None):
        y_copies.update(
            exchange(trio, down, lambda p, u, v: yr[p].at[u, v], y_send, y_recv, prepare)
        )

    give_back(RETURNS[0][:2], second_half)
    lax.fori_loop(0, SIDE, reorder_last, 0)
    give_back(RETURNS[0][2:])
    for trio in RETURNS[1:]:
        give_back(trio)

    for copy in l_copies.values():
        copy.wait_send()
    for copy in m_copies.values():
        copy.wait_send()
    p_copies, z_copies = {}, {}
    half = SIDE * tokens

    def share(p):
        band, first = SHARES[p]
        return acc.at[half * band:half * (band + 1), first:first + PIECES[p][2]]

    def part(p, o):
        rows = pl.ds(pl.multiple_of(o * half, half), half)
        return jnp.dot(
            sel[PIECES[p][0], rows, :], yr[p][...].reshape(total, PIECES[p][2]),
            preferred_element_type=F32,
        )

    def combine(trio):
        for p in trio:
            for i, j in PEERS:
                y_copies[p, i, j].wait()
            tokg[p][:, 0] = part(p, 1 - core).astype(BF16).reshape(SIDE, tokens, PIECES[p][2])
            copy = remote(
                tokg[p].at[:, 0], pr[p], p_send.at[p], p_recv.at[p], device((0, 0, 0), 1 - core)
            )
            copy.start()
            p_copies[p] = copy
        for p in trio:
            share(p)[...] = part(p, core)

    def reduce_cores(p):
        t, first, width = PIECES[p]
        p_copies[p].wait()
        both = share(p)[...] + pr[p][...].reshape(half, width).astype(F32)
        share(p)[...] = both
        tokg[p][:, 1] = both.astype(BF16).reshape(SIDE, tokens, width)
        for d in LINE:
            copy = remote(
                tokg[p].at[near[t][d], 1], zr[p].at[d - 1],
                z_send.at[p, d], z_recv.at[p, d], device(on_line(t, d), core),
            )
            copy.start()
            z_copies[p, d] = copy

    def finish(p):
        t, first, width = PIECES[p]
        result = share(p)[pl.ds(pl.multiple_of(here[t] * tokens, tokens), tokens), :]
        for d in LINE:
            z_copies[p, d].wait()
        for d in range(1, SIDE):
            result = result + zr[p][d - 1].astype(F32)
        out_ref[:, first:first + width] = result.astype(BF16)

    for k, trio in enumerate(RETURNS):
        combine(trio)
        for p in trio:
            reduce_cores(p)
        if k == 1:
            for p in RETURNS[0]:
                finish(p)
    for trio in RETURNS[1:]:
        for p in trio:
            finish(p)


def body(tokens, expert_ids, gate_probs, w_gate, w_up, w_down):
    count, choices = expert_ids.shape
    width = tokens.shape[1]
    hidden = w_gate.shape[2]
    slots = 10
    group = 2 * SIDE * slots
    total = SIDE * SIDE * group
    n = len(PIECES)
    any_spec = pl.BlockSpec(memory_space=pl.ANY)
    dma = pltpu.SemaphoreType.DMA
    widths = [w for _, _, w in PIECES]
    scratch = (
        [pltpu.VMEM((SIDE, 2, count, w), BF16) for w in widths]
        + [pltpu.VMEM((SIDE, SIDE, group, w), BF16) for w in widths]
        + [pltpu.VMEM((SIDE, SIDE, group, w), BF16) for w in widths]
        + [pltpu.VMEM((SIDE, count, w), BF16) for w in widths]
        + [pltpu.VMEM((SIDE - 1, count, w), BF16) for w in widths]
        + [
            pltpu.VMEM((choices, count), jnp.int32),
            pltpu.VMEM((choices, count), F32),
            pltpu.VMEM((width, hidden), BF16),
            pltpu.VMEM((width, hidden), BF16),
            pltpu.VMEM((hidden, width), BF16),
            pltpu.VMEM((3, SIDE, 2, 2, 16, count), BF16),
            pltpu.VMEM((3, 2 * SIDE, 2, 16, count), BF16),
            pltpu.VMEM((16, count), F32),
            pltpu.VMEM((3, total, total), BF16),
            pltpu.VMEM((SIDE * group, SIDE * group), BF16),
            pltpu.VMEM((16, total), BF16),
            pltpu.VMEM((SIDE, SIDE, group, width), BF16),
            pltpu.VMEM((total, 2 * hidden), F32),
            pltpu.VMEM((SIDE, SIDE, group, hidden), BF16),
            pltpu.VMEM((2, SIDE, SIDE, group, hidden), BF16),
            dma((5 + n,)),
            pltpu.SemaphoreType.REGULAR((2,)),
            dma((3, SIDE, 2)), dma((3, SIDE, 2)),
            dma((n, SIDE)), dma((n, SIDE)),
            dma((n, SIDE)), dma((n, SIDE)),
            dma((n, SIDE, SIDE)), dma((n, SIDE, SIDE)),
            dma((n, SIDE, SIDE)), dma((n, SIDE, SIDE)),
            dma((n,)), dma((n,)),
            dma((n, SIDE)), dma((n, SIDE)),
        ]
    )
    return pl.pallas_call(
        functools.partial(moe_kernel, slots),
        out_shape=jax.ShapeDtypeStruct((count, width), BF16),
        in_specs=[any_spec] * 6,
        out_specs=pl.BlockSpec(memory_space=pltpu.VMEM),
        scratch_shapes=scratch,
        compiler_params=pltpu.CompilerParams(
            collective_id=0, has_side_effects=True, vmem_limit_bytes=67043328
        ),
    )(expert_ids.T, gate_probs.T, tokens, w_gate, w_up, w_down)


def solution(mesh):
    in_specs = (
        P(("row", "col"), None),
        P(("row", "col"), None),
        P(("row", "col"), None),
        P(("row", "col"), None, None),
        P(("row", "col"), None, None),
        P(("row", "col"), None, None),
    )
    out_specs = P(("row", "col"), None)
    return jax.shard_map(body, mesh=mesh, in_specs=in_specs, out_specs=out_specs, check_vma=False)
```

```python
import functools

import jax
import jax.numpy as jnp
from jax import lax
from jax.experimental import pallas as pl
from jax.experimental.pallas import tpu as pltpu
from jax.sharding import PartitionSpec as P

MESH = pl.DeviceIdType.MESH
BF16 = jnp.bfloat16
F32 = jnp.float32
SIDE = 4
PIECES = (
    (0, 0, 128), (1, 128, 128), (2, 256, 128),
    (0, 384, 384), (1, 768, 256), (2, 1024, 256),
    (0, 1280, 256), (1, 1536, 256), (2, 1792, 256),
)
TRIOS = ((0, 1, 2), (3, 4, 5), (6, 7, 8))
RETURNS = (TRIOS[1], TRIOS[2], TRIOS[0])
HALF = 1280
SHARES = ((0, 896), (0, 1024), (0, 1152), (0, 0), (0, 384), (0, 640), (1, 0), (1, 256), (1, 512))
PLANES = ((2, 1), (2, 0), (0, 1))
PEERS = tuple((i, j) for i in range(SIDE) for j in range(SIDE) if i or j)
LINE = (2, 1, 3)
UNNAMED = -1024.0


def moe_kernel(
    slots,
    ids_in, probs_in, tok_in, wg_in, wu_in, wd_in, out_ref, *scratch,
):
    n = len(PIECES)
    tokg, scratch = scratch[:n], scratch[n:]
    xs, scratch = scratch[:n], scratch[n:]
    yr, scratch = scratch[:n], scratch[n:]
    pr, scratch = scratch[:n], scratch[n:]
    zr, scratch = scratch[:n], scratch[n:]
    (
        ids, probs, wg, wu, wd, kw_out, kw_in, kf, sel, swap, spread, xc, acc, hid, hidp,
        load_sem, ready, k_send, k_recv, l_send, l_recv, m_send, m_recv, x_send, x_recv,
        y_send, y_recv, p_send, p_recv, z_send, z_recv,
    ) = scratch
    r = lax.axis_index("row")
    c = lax.axis_index("col")
    core = c % 2
    sign = 1 - 2 * core
    here = (r % SIDE, (c // 2) % SIDE, 2 * (r // SIDE) + c // 8)
    near = [[(h + sign * d + SIDE) % SIDE for d in range(SIDE)] for h in here]
    row_x = near[0]
    col_y = [2 * v for v in near[1]]
    row_z = [SIDE * (v // 2) for v in near[2]]
    col_z = [8 * (v % 2) for v in near[2]]
    tokens = tok_in.shape[0]
    hidden = wg.shape[1]
    group = 2 * SIDE * slots
    slab = SIDE * group
    total = SIDE * slab

    def device(d, to_core):
        return (row_z[d[2]] + row_x[d[0]], col_z[d[2]] + col_y[d[1]] + to_core)

    def remote(src, dst, send, recv, to):
        return pltpu.make_async_remote_copy(
            src_ref=src, dst_ref=dst, send_sem=send, recv_sem=recv,
            device_id=to, device_id_type=MESH,
        )

    def on_line(t, d):
        step = [0, 0, 0]
        step[t] = d
        return tuple(step)

    def in_plane(t, i, j):
        step = [0, 0, 0]
        step[PLANES[t][0]] = i
        step[PLANES[t][1]] = j
        return tuple(step)

    load_ids = pltpu.make_async_copy(ids_in, ids, load_sem.at[0])
    load_probs = pltpu.make_async_copy(probs_in, probs, load_sem.at[1])
    load_ids.start()
    load_probs.start()
    load_tok = []
    for p, (t, first, width) in enumerate(PIECES):
        copy = pltpu.make_async_copy(
            tok_in.at[:, pl.ds(first, width)], tokg[p].at[here[t], core], load_sem.at[5 + p]
        )
        copy.start()
        load_tok.append(copy)
    barrier = pltpu.get_barrier_semaphore()

    def greet(semaphore, to):
        pl.semaphore_signal(semaphore, inc=1, device_id=to, device_id_type=MESH)

    greet(barrier, device((0, 0, 0), 1 - core))
    for d in LINE:
        for t in range(3):
            greet(barrier, device(on_line(t, d), core))

    load_ids.wait()
    load_probs.wait()
    load_w = [
        pltpu.make_async_copy(wg_in.at[0], wg, load_sem.at[2]),
        pltpu.make_async_copy(wu_in.at[0], wu, load_sem.at[3]),
        pltpu.make_async_copy(wd_in.at[0], wd, load_sem.at[4]),
    ]
    experts = ids.shape[0] * 16
    place = lax.broadcasted_iota(jnp.int32, (experts, tokens), 0)
    line_of = jnp.right_shift(place, 5)
    core_of = jnp.bitwise_and(jnp.right_shift(place, 4), 1)
    slow_of = jnp.bitwise_and(jnp.right_shift(place, 2), 3)
    fast_of = jnp.bitwise_and(place, 3)
    earlier = (
        lax.broadcasted_iota(jnp.int32, (tokens, tokens), 0)
        < lax.broadcasted_iota(jnp.int32, (tokens, tokens), 1)
    ).astype(BF16)
    for t in range(3):
        at = [None] * 3
        at[t], at[PLANES[t][0]], at[PLANES[t][1]] = line_of, slow_of, fast_of
        expert = (
            16 * (SIDE * jnp.right_shift(at[2], 1) + at[0])
            + 8 * jnp.bitwise_and(at[2], 1) + 2 * at[1] + core_of
        )
        named = jnp.zeros((experts, tokens), F32)
        weight = jnp.zeros((experts, tokens), F32)
        for k in range(ids.shape[0]):
            hit = ids[k:k + 1, :] == expert
            named = jnp.where(hit, 1.0, named)
            weight = jnp.where(hit, probs[k:k + 1, :], weight)
        rank = jnp.dot(named.astype(BF16), earlier, preferred_element_type=F32)
        key = jnp.where(named > 0.5, rank, UNNAMED).astype(BF16)
        weight = weight.astype(BF16)
        for l in range(SIDE):
            for o in range(2):
                rows = slice((2 * l + o) * 16, (2 * l + o + 1) * 16)
                kw_out[t, l, o, 0] = key[rows]
                kw_out[t, l, o, 1] = weight[rows]
        kw_in[t, 2 * here[t] + core] = kw_out[t, here[t], core]

    pl.semaphore_wait(barrier, 1 + 3 * len(LINE))
    greet(ready.at[0], device((0, 0, 0), 1 - core))
    for d in LINE:
        for t in range(3):
            greet(ready.at[1], device(on_line(t, d), core))

    k_copies = {}

    def send_keys(t, d, o):
        to_core = core if o == 0 else 1 - core
        copy = remote(
            kw_out.at[t, near[t][d], to_core], kw_in.at[t, 2 * here[t] + core],
            k_send.at[t, d, o], k_recv.at[t, d, o], device(on_line(t, d), to_core),
        )
        copy.start()
        k_copies[t, d, o] = copy

    l_copies = {}
    m_copies = {}

    def to_mate(p, d):
        t = PIECES[p][0]
        block = tokg[p].at[near[t][(SIDE - d) % SIDE], core]
        copy = remote(
            block, block, m_send.at[p, d], m_recv.at[p, d], device((0, 0, 0), 1 - core)
        )
        copy.start()
        m_copies[p, d] = copy

    def send_tokens(trio):
        for p in trio:
            load_tok[p].wait()
        for d in LINE:
            for p in trio:
                t = PIECES[p][0]
                block = tokg[p].at[here[t], core]
                copy = remote(
                    block, block, l_send.at[p, d], l_recv.at[p, d], device(on_line(t, d), core)
                )
                copy.start()
                l_copies[p, d] = copy
        for p in trio:
            to_mate(p, 0)

    for t in range(3):
        for d in LINE:
            send_keys(t, d, 0)
        send_keys(t, 0, 1)
    send_tokens(TRIOS[0])
    pl.semaphore_wait(ready.at[0], 1)
    for t in range(3):
        for d in LINE:
            send_keys(t, d, 1)
    for trio in TRIOS[1:]:
        send_tokens(trio)
    for copy in load_w:
        copy.start()

    row_id = lax.broadcasted_iota(jnp.int32, (slab, slab), 0)
    col_id = lax.broadcasted_iota(jnp.int32, (slab, slab), 1)
    pair = 2 * slots
    twin = jnp.zeros((slab, slab), jnp.int32)
    for i in range(SIDE):
        for j in range(SIDE):
            first = (i * SIDE + j) * pair
            twin = jnp.where(
                (col_id >= first) & (col_id < first + pair),
                col_id + ((j * SIDE + i) * pair - first), twin,
            )
    swap[...] = (row_id == twin).astype(F32).astype(BF16)
    lane = lax.broadcasted_iota(jnp.int32, (16, total), 1)
    owner = group * lax.broadcasted_iota(jnp.int32, (16, total), 0)
    spread[...] = ((lane >= owner) & (lane < owner + group)).astype(F32).astype(BF16)

    def forward(p):
        for d in LINE:
            l_copies[p, d].wait_recv()
            to_mate(p, d)

    slot_of = lax.broadcasted_iota(jnp.int32, (group, tokens), 0).astype(F32)
    for t in range(3):
        def choose(s, _):
            kf[...] = kw_in[t, s, 0].astype(F32) + (s * slots).astype(F32)
            lanes = pl.ds(pl.multiple_of(s * tokens, tokens), tokens)
            for q in range(SIDE * SIDE):
                sel[t, q * group:(q + 1) * group, lanes] = (
                    slot_of == kf[q:q + 1, :]
                ).astype(F32).astype(BF16)
            return 0

        for (kind, d, o), copy in k_copies.items():
            if kind == t:
                copy.wait()
        lax.fori_loop(0, 2 * SIDE, choose, 0)
        if t == 0:
            for p in TRIOS[0]:
                forward(p)

    def exchange(trio, product, landing, send, recv, prepare=None):
        copies = {}

        def peer(p, i, j, v):
            a, b = PLANES[PIECES[p][0]]
            at = list(here)
            at[a], at[b] = v, near[b][j]
            return remote(
                xs[p].at[v, near[b][j]], landing(p, here[a], here[b]),
                send.at[p, i, j], recv.at[p, i, j],
                (SIDE * (at[2] // 2) + at[0], 8 * (at[2] % 2) + 2 * at[1] + core),
            )

        def slab_of(i, _):
            where = []
            if prepare is not None:
                prepare((here[PLANES[PIECES[trio[0]][0]][0]] + sign * i + SIDE) % SIDE)
            for p in trio:
                v = (here[PLANES[PIECES[p][0]][0]] + sign * i + SIDE) % SIDE
                xs[p][v] = product(p, v).astype(BF16).reshape(SIDE, group, PIECES[p][2])
                where.append(v)

            @pl.when(i > 0)
            def _():
                for p, v in zip(trio, where):
                    peer(p, i, 0, v).start()

            for j in range(1, SIDE):
                for p, v in zip(trio, where):
                    peer(p, i, j, v).start()
            return 0

        lax.fori_loop(0, SIDE, slab_of, 0)
        for p in trio:
            a, b = PLANES[PIECES[p][0]]
            landing(p, here[a], here[b])[...] = xs[p][here[a], here[b]]
            for i, j in PEERS:
                copies[p, i, j] = peer(p, i, j, near[a][i])
        return copies

    sources = 2 * SIDE * tokens
    x_copies = {}

    def select(p, v):
        t, first, width = PIECES[p]
        rows = pl.ds(pl.multiple_of(v * slab, slab), slab)
        return jnp.dot(
            sel[t, rows, :sources], tokg[p][...].reshape(sources, width),
            preferred_element_type=F32,
        )

    def arrival(p, u, v):
        return xc.at[u, v, :, pl.ds(PIECES[p][1], PIECES[p][2])]

    for trio in TRIOS:
        for p in trio:
            for d in range(SIDE):
                m_copies[p, d].wait_recv()
        if trio == TRIOS[0]:
            pl.semaphore_wait(ready.at[1], 3 * len(LINE))
        x_copies.update(exchange(trio, select, arrival, x_send, x_recv))
        if trio != TRIOS[-1]:
            for p in TRIOS[TRIOS.index(trio) + 1]:
                forward(p)

    lane = lax.broadcasted_iota(jnp.int32, (1, total), 1)
    slot_at = lane
    for q in range(1, SIDE * SIDE):
        slot_at = jnp.where(lane >= q * group, lane - q * group, slot_at)
    slot_at = slot_at.astype(F32)
    for t in range(3):
        def weigh(s, _):
            expand = lambda w: lax.dot_general(
                kw_in[t, s, w], spread[...], (((0,), (0,)), ((), ())),
                preferred_element_type=F32,
            )
            chosen = expand(0) + (s * slots).astype(F32) == slot_at
            value = jnp.where(chosen, expand(1), 0.0).astype(BF16)
            o, l = s // SIDE, s % SIDE
            return value

        def weigh_all(l, _):
            for o in range(2):
                rows = pl.ds(pl.multiple_of((o * SIDE + l) * tokens, tokens), tokens)
                sel[t, rows, :] = weigh(2 * l + o, 0)
            return 0

        lax.fori_loop(0, SIDE, weigh_all, 0)

    def arrive(p):
        for i, j in PEERS:
            x_copies[p, i, j].wait()

    def reorder(p, i):
        t, first, width = PIECES[p]
        block = xc.at[i] if t == 1 else xc.at[:, i]
        columns = pl.ds(first, width)
        res = jnp.dot(
            swap[...], block[:, :, columns].reshape(slab, width), preferred_element_type=F32
        )
        block[:, :, columns] = res.astype(BF16).reshape(SIDE, group, width)

    def reorder_all(p):
        def one(i, _):
            reorder(p, i)
            return 0

        lax.fori_loop(0, SIDE, one, 0)

    f_tile = 256
    m_rows = 2 * slab

    def first_half(k, _):
        f = pl.multiple_of(k * f_tile, f_tile)
        for m in range(2):
            x = xc[2 * m:2 * m + 2, :, :, :HALF].reshape(m_rows, HALF)
            rows = slice(m * m_rows, (m + 1) * m_rows)
            acc[rows, pl.ds(f, f_tile)] = jnp.dot(
                x, wg[:HALF, pl.ds(f, f_tile)], preferred_element_type=F32
            )
            acc[rows, pl.ds(hidden + f, f_tile)] = jnp.dot(
                x, wu[:HALF, pl.ds(f, f_tile)], preferred_element_type=F32
            )
        return 0

    def reorder_hidden(t, i):
        src = hid.at[i] if t == 1 else hid.at[:, i]
        dst = hidp.at[t - 1, i] if t == 1 else hidp.at[t - 1, :, i]
        res = jnp.dot(swap[...], src[...].reshape(slab, hidden), preferred_element_type=F32)
        dst[...] = res.astype(BF16).reshape(SIDE, group, hidden)

    def second_half(v):
        reorder(TRIOS[2][1], v)
        rows = pl.ds(pl.multiple_of(v * slab, slab), slab)

        def one(k, _):
            f = pl.multiple_of(k * f_tile, f_tile)
            x = xc[v, :, :, HALF:]
            x = x.reshape(slab, x.shape[-1])
            gate = acc[rows, pl.ds(f, f_tile)] + jnp.dot(
                x, wg[HALF:, pl.ds(f, f_tile)], preferred_element_type=F32
            )
            up = acc[rows, pl.ds(hidden + f, f_tile)] + jnp.dot(
                x, wu[HALF:, pl.ds(f, f_tile)], preferred_element_type=F32
            )
            value = (gate / (1.0 + jnp.exp(-gate)) * up).astype(BF16)
            hid[v, :, :, pl.ds(f, f_tile)] = value.reshape(SIDE, group, f_tile)
            return 0

        lax.fori_loop(0, hidden // f_tile, one, 0)
        reorder_hidden(1, v)

    for p in TRIOS[0] + TRIOS[1]:
        arrive(p)
        if PIECES[p][0] > 0:
            reorder_all(p)
    for copy in load_w:
        copy.wait()
    lax.fori_loop(0, hidden // f_tile, first_half, 0)
    for p in TRIOS[2]:
        arrive(p)
    reorder_all(TRIOS[2][2])

    y_copies = {}

    def down(p, v):
        t, first, width = PIECES[p]
        source = hid if t == 0 else hidp.at[t - 1]
        return jnp.dot(
            source[v].reshape(slab, hidden), wd[:, first:first + width],
            preferred_element_type=F32,
        )

    def reorder_last(i, _):
        reorder_hidden(2, i)
        return 0

    def give_back(trio, prepare=None):
        y_copies.update(
            exchange(trio, down, lambda p, u, v: yr[p].at[u, v], y_send, y_recv, prepare)
        )

    give_back(RETURNS[0][:2], second_half)
    lax.fori_loop(0, SIDE, reorder_last, 0)
    give_back(RETURNS[0][2:])
    for trio in RETURNS[1:]:
        give_back(trio)

    for copy in l_copies.values():
        copy.wait_send()
    for copy in m_copies.values():
        copy.wait_send()
    p_copies, z_copies = {}, {}
    half = SIDE * tokens

    def share(p):
        band, first = SHARES[p]
        return acc.at[half * band:half * (band + 1), first:first + PIECES[p][2]]

    def part(p, o):
        rows = pl.ds(pl.multiple_of(o * half, half), half)
        return jnp.dot(
            sel[PIECES[p][0], rows, :], yr[p][...].reshape(total, PIECES[p][2]),
            preferred_element_type=F32,
        )

    def combine(trio):
        for p in trio:
            for i, j in PEERS:
                y_copies[p, i, j].wait()
            tokg[p][:, 0] = part(p, 1 - core).astype(BF16).reshape(SIDE, tokens, PIECES[p][2])
            copy = remote(
                tokg[p].at[:, 0], pr[p], p_send.at[p], p_recv.at[p], device((0, 0, 0), 1 - core)
            )
            copy.start()
            p_copies[p] = copy
        for p in trio:
            share(p)[...] = part(p, core)

    def reduce_cores(p):
        t, first, width = PIECES[p]
        p_copies[p].wait()
        both = share(p)[...] + pr[p][...].reshape(half, width).astype(F32)
        tokg[p][:, 1] = both.astype(BF16).reshape(SIDE, tokens, width)
        for d in LINE:
            copy = remote(
                tokg[p].at[near[t][d], 1], zr[p].at[d - 1],
                z_send.at[p, d], z_recv.at[p, d], device(on_line(t, d), core),
            )
            copy.start()
            z_copies[p, d] = copy

    def finish(p):
        t, first, width = PIECES[p]
        result = share(p)[pl.ds(pl.multiple_of(here[t] * tokens, tokens), tokens), :]
        result = result + pr[p][here[t]].astype(F32)
        for d in LINE:
            z_copies[p, d].wait()
        for d in range(1, SIDE):
            result = result + zr[p][d - 1].astype(F32)
        out_ref[:, first:first + width] = result.astype(BF16)

    for k, trio in enumerate(RETURNS):
        combine(trio)
        for p in trio:
            reduce_cores(p)
        if k == 1:
            for p in RETURNS[0]:
                finish(p)
    for trio in RETURNS[1:]:
        for p in trio:
            finish(p)


def body(tokens, expert_ids, gate_probs, w_gate, w_up, w_down):
    count, choices = expert_ids.shape
    width = tokens.shape[1]
    hidden = w_gate.shape[2]
    slots = 10
    group = 2 * SIDE * slots
    total = SIDE * SIDE * group
    n = len(PIECES)
    any_spec = pl.BlockSpec(memory_space=pl.ANY)
    dma = pltpu.SemaphoreType.DMA
    widths = [w for _, _, w in PIECES]
    scratch = (
        [pltpu.VMEM((SIDE, 2, count, w), BF16) for w in widths]
        + [pltpu.VMEM((SIDE, SIDE, group, w), BF16) for w in widths]
        + [pltpu.VMEM((SIDE, SIDE, group, w), BF16) for w in widths]
        + [pltpu.VMEM((SIDE, count, w), BF16) for w in widths]
        + [pltpu.VMEM((SIDE - 1, count, w), BF16) for w in widths]
        + [
            pltpu.VMEM((choices, count), jnp.int32),
            pltpu.VMEM((choices, count), F32),
            pltpu.VMEM((width, hidden), BF16),
            pltpu.VMEM((width, hidden), BF16),
            pltpu.VMEM((hidden, width), BF16),
            pltpu.VMEM((3, SIDE, 2, 2, 16, count), BF16),
            pltpu.VMEM((3, 2 * SIDE, 2, 16, count), BF16),
            pltpu.VMEM((16, count), F32),
            pltpu.VMEM((3, total, total), BF16),
            pltpu.VMEM((SIDE * group, SIDE * group), BF16),
            pltpu.VMEM((16, total), BF16),
            pltpu.VMEM((SIDE, SIDE, group, width), BF16),
            pltpu.VMEM((total, 2 * hidden), F32),
            pltpu.VMEM((SIDE, SIDE, group, hidden), BF16),
            pltpu.VMEM((2, SIDE, SIDE, group, hidden), BF16),
            dma((5 + n,)),
            pltpu.SemaphoreType.REGULAR((2,)),
            dma((3, SIDE, 2)), dma((3, SIDE, 2)),
            dma((n, SIDE)), dma((n, SIDE)),
            dma((n, SIDE)), dma((n, SIDE)),
            dma((n, SIDE, SIDE)), dma((n, SIDE, SIDE)),
            dma((n, SIDE, SIDE)), dma((n, SIDE, SIDE)),
            dma((n,)), dma((n,)),
            dma((n, SIDE)), dma((n, SIDE)),
        ]
    )
    return pl.pallas_call(
        functools.partial(moe_kernel, slots),
        out_shape=jax.ShapeDtypeStruct((count, width), BF16),
        in_specs=[any_spec] * 6,
        out_specs=pl.BlockSpec(memory_space=pltpu.VMEM),
        scratch_shapes=scratch,
        compiler_params=pltpu.CompilerParams(
            collective_id=0, has_side_effects=True, vmem_limit_bytes=67043328
        ),
    )(expert_ids.T, gate_probs.T, tokens, w_gate, w_up, w_down)


def solution(mesh):
    in_specs = (
        P(("row", "col"), None),
        P(("row", "col"), None),
        P(("row", "col"), None),
        P(("row", "col"), None, None),
        P(("row", "col"), None, None),
        P(("row", "col"), None, None),
    )
    out_specs = P(("row", "col"), None)
    return jax.shard_map(body, mesh=mesh, in_specs=in_specs, out_specs=out_specs, check_vma=False)
```

```python
import functools

import jax
import jax.numpy as jnp
from jax import lax
from jax.experimental import pallas as pl
from jax.experimental.pallas import tpu as pltpu
from jax.sharding import PartitionSpec as P

MESH = pl.DeviceIdType.MESH
BF16 = jnp.bfloat16
F32 = jnp.float32
SIDE = 4
PIECES = (
    (0, 0, 128), (1, 128, 128), (2, 256, 128),
    (0, 384, 384), (1, 768, 256), (2, 1024, 256),
    (0, 1280, 256), (1, 1536, 256), (2, 1792, 256),
)
TRIOS = ((0, 1, 2), (3, 4, 5), (6, 7, 8))
RETURNS = (TRIOS[1], TRIOS[2], TRIOS[0])
HALF = 1280
SHARES = ((0, 896), (0, 1024), (0, 1152), (0, 0), (0, 384), (0, 640), (1, 0), (1, 256), (1, 512))
PLANES = ((2, 1), (2, 0), (0, 1))
PEERS = tuple((i, j) for i in range(SIDE) for j in range(SIDE) if i or j)
LINE = (2, 1, 3)
UNNAMED = -1024.0


def moe_kernel(
    slots,
    ids_in, probs_in, tok_in, wg_in, wu_in, wd_in, out_ref, *scratch,
):
    n = len(PIECES)
    tokg, scratch = scratch[:n], scratch[n:]
    xs, scratch = scratch[:n], scratch[n:]
    yr, scratch = scratch[:n], scratch[n:]
    pr, scratch = scratch[:n], scratch[n:]
    zr, scratch = scratch[:n], scratch[n:]
    (
        ids, probs, wg, wu, wd, kw_out, kw_in, kf, sel, swap, spread, xc, acc, hid, hidp,
        load_sem, ready, k_send, k_recv, l_send, l_recv, m_send, m_recv, x_send, x_recv,
        y_send, y_recv, p_send, p_recv, z_send, z_recv,
    ) = scratch
    r = lax.axis_index("row")
    c = lax.axis_index("col")
    core = c % 2
    sign = 1 - 2 * core
    here = (r % SIDE, (c // 2) % SIDE, 2 * (r // SIDE) + c // 8)
    near = [[(h + sign * d + SIDE) % SIDE for d in range(SIDE)] for h in here]
    row_x = near[0]
    col_y = [2 * v for v in near[1]]
    row_z = [SIDE * (v // 2) for v in near[2]]
    col_z = [8 * (v % 2) for v in near[2]]
    tokens = tok_in.shape[0]
    hidden = wg.shape[1]
    group = 2 * SIDE * slots
    slab = SIDE * group
    total = SIDE * slab

    def device(d, to_core):
        return (row_z[d[2]] + row_x[d[0]], col_z[d[2]] + col_y[d[1]] + to_core)

    def remote(src, dst, send, recv, to):
        return pltpu.make_async_remote_copy(
            src_ref=src, dst_ref=dst, send_sem=send, recv_sem=recv,
            device_id=to, device_id_type=MESH,
        )

    def on_line(t, d):
        step = [0, 0, 0]
        step[t] = d
        return tuple(step)

    def in_plane(t, i, j):
        step = [0, 0, 0]
        step[PLANES[t][0]] = i
        step[PLANES[t][1]] = j
        return tuple(step)

    load_ids = pltpu.make_async_copy(ids_in, ids, load_sem.at[0])
    load_probs = pltpu.make_async_copy(probs_in, probs, load_sem.at[1])
    load_ids.start()
    load_probs.start()
    load_tok = []
    for p, (t, first, width) in enumerate(PIECES):
        copy = pltpu.make_async_copy(
            tok_in.at[:, pl.ds(first, width)], tokg[p].at[here[t], core], load_sem.at[5 + p]
        )
        copy.start()
        load_tok.append(copy)
    barrier = pltpu.get_barrier_semaphore()

    def greet(semaphore, to):
        pl.semaphore_signal(semaphore, inc=1, device_id=to, device_id_type=MESH)

    greet(barrier, device((0, 0, 0), 1 - core))
    for d in LINE:
        for t in range(3):
            greet(barrier, device(on_line(t, d), core))

    load_ids.wait()
    load_probs.wait()
    load_w = [
        pltpu.make_async_copy(wg_in.at[0], wg, load_sem.at[2]),
        pltpu.make_async_copy(wu_in.at[0], wu, load_sem.at[3]),
        pltpu.make_async_copy(wd_in.at[0], wd, load_sem.at[4]),
    ]
    experts = ids.shape[0] * 16
    place = lax.broadcasted_iota(jnp.int32, (experts, tokens), 0)
    line_of = jnp.right_shift(place, 5)
    core_of = jnp.bitwise_and(jnp.right_shift(place, 4), 1)
    slow_of = jnp.bitwise_and(jnp.right_shift(place, 2), 3)
    fast_of = jnp.bitwise_and(place, 3)
    earlier = (
        lax.broadcasted_iota(jnp.int32, (tokens, tokens), 0)
        < lax.broadcasted_iota(jnp.int32, (tokens, tokens), 1)
    ).astype(BF16)
    for t in range(3):
        at = [None] * 3
        at[t], at[PLANES[t][0]], at[PLANES[t][1]] = line_of, slow_of, fast_of
        expert = (
            16 * (SIDE * jnp.right_shift(at[2], 1) + at[0])
            + 8 * jnp.bitwise_and(at[2], 1) + 2 * at[1] + core_of
        )
        named = jnp.zeros((experts, tokens), F32)
        weight = jnp.zeros((experts, tokens), F32)
        for k in range(ids.shape[0]):
            hit = ids[k:k + 1, :] == expert
            named = jnp.where(hit, 1.0, named)
            weight = jnp.where(hit, probs[k:k + 1, :], weight)
        rank = jnp.dot(named.astype(BF16), earlier, preferred_element_type=F32)
        key = jnp.where(named > 0.5, rank, UNNAMED).astype(BF16)
        weight = weight.astype(BF16)
        for l in range(SIDE):
            for o in range(2):
                rows = slice((2 * l + o) * 16, (2 * l + o + 1) * 16)
                kw_out[t, l, o, 0] = key[rows]
                kw_out[t, l, o, 1] = weight[rows]
        kw_in[t, 2 * here[t] + core] = kw_out[t, here[t], core]

    pl.semaphore_wait(barrier, 1 + 3 * len(LINE))
    greet(ready.at[0], device((0, 0, 0), 1 - core))
    for d in LINE:
        for t in range(3):
            greet(ready.at[1], device(on_line(t, d), core))

    k_copies = {}

    def send_keys(t, d, o):
        to_core = core if o == 0 else 1 - core
        copy = remote(
            kw_out.at[t, near[t][d], to_core], kw_in.at[t, 2 * here[t] + core],
            k_send.at[t, d, o], k_recv.at[t, d, o], device(on_line(t, d), to_core),
        )
        copy.start()
        k_copies[t, d, o] = copy

    l_copies = {}
    m_copies = {}

    def to_mate(p, d):
        t = PIECES[p][0]
        block = tokg[p].at[near[t][(SIDE - d) % SIDE], core]
        copy = remote(
            block, block, m_send.at[p, d], m_recv.at[p, d], device((0, 0, 0), 1 - core)
        )
        copy.start()
        m_copies[p, d] = copy

    def send_tokens(trio):
        for p in trio:
            load_tok[p].wait()
        for d in LINE:
            for p in trio:
                t = PIECES[p][0]
                block = tokg[p].at[here[t], core]
                copy = remote(
                    block, block, l_send.at[p, d], l_recv.at[p, d], device(on_line(t, d), core)
                )
                copy.start()
                l_copies[p, d] = copy
        for p in trio:
            to_mate(p, 0)

    for t in range(3):
        for d in LINE:
            send_keys(t, d, 0)
        send_keys(t, 0, 1)
    send_tokens(TRIOS[0])
    pl.semaphore_wait(ready.at[0], 1)
    for t in range(3):
        for d in LINE:
            send_keys(t, d, 1)
    for trio in TRIOS[1:]:
        send_tokens(trio)
    for copy in load_w:
        copy.start()

    row_id = lax.broadcasted_iota(jnp.int32, (slab, slab), 0)
    col_id = lax.broadcasted_iota(jnp.int32, (slab, slab), 1)
    pair = 2 * slots
    twin = jnp.zeros((slab, slab), jnp.int32)
    for i in range(SIDE):
        for j in range(SIDE):
            first = (i * SIDE + j) * pair
            twin = jnp.where(
                (col_id >= first) & (col_id < first + pair),
                col_id + ((j * SIDE + i) * pair - first), twin,
            )
    swap[...] = (row_id == twin).astype(F32).astype(BF16)
    lane = lax.broadcasted_iota(jnp.int32, (16, total), 1)
    owner = group * lax.broadcasted_iota(jnp.int32, (16, total), 0)
    spread[...] = ((lane >= owner) & (lane < owner + group)).astype(F32).astype(BF16)

    def forward(p):
        for d in LINE:
            l_copies[p, d].wait_recv()
            to_mate(p, d)

    slot_of = lax.broadcasted_iota(jnp.int32, (group, tokens), 0).astype(F32)
    for t in range(3):
        def choose(s, _):
            kf[...] = kw_in[t, s, 0].astype(F32) + (s * slots).astype(F32)
            lanes = pl.ds(pl.multiple_of(s * tokens, tokens), tokens)
            for q in range(SIDE * SIDE):
                sel[t, q * group:(q + 1) * group, lanes] = (
                    slot_of == kf[q:q + 1, :]
                ).astype(F32).astype(BF16)
            return 0

        for (kind, d, o), copy in k_copies.items():
            if kind == t:
                copy.wait()
        lax.fori_loop(0, 2 * SIDE, choose, 0)
        if t == 0:
            for p in TRIOS[0]:
                forward(p)

    def exchange(trio, product, landing, send, recv, prepare=None):
        copies = {}

        def peer(p, i, j, v):
            a, b = PLANES[PIECES[p][0]]
            at = list(here)
            at[a], at[b] = v, near[b][j]
            return remote(
                xs[p].at[v, near[b][j]], landing(p, here[a], here[b]),
                send.at[p, i, j], recv.at[p, i, j],
                (SIDE * (at[2] // 2) + at[0], 8 * (at[2] % 2) + 2 * at[1] + core),
            )

        def slab_of(i, _):
            where = []
            if prepare is not None:
                prepare((here[PLANES[PIECES[trio[0]][0]][0]] + sign * i + SIDE) % SIDE)
            for p in trio:
                v = (here[PLANES[PIECES[p][0]][0]] + sign * i + SIDE) % SIDE
                xs[p][v] = product(p, v).astype(BF16).reshape(SIDE, group, PIECES[p][2])
                where.append(v)

            @pl.when(i > 0)
            def _():
                for p, v in zip(trio, where):
                    peer(p, i, 0, v).start()

            for j in range(1, SIDE):
                for p, v in zip(trio, where):
                    peer(p, i, j, v).start()
            return 0

        lax.fori_loop(0, SIDE, slab_of, 0)
        for p in trio:
            a, b = PLANES[PIECES[p][0]]
            landing(p, here[a], here[b])[...] = xs[p][here[a], here[b]]
            for i, j in PEERS:
                copies[p, i, j] = peer(p, i, j, near[a][i])
        return copies

    sources = 2 * SIDE * tokens
    x_copies = {}

    def select(p, v):
        t, first, width = PIECES[p]
        rows = pl.ds(pl.multiple_of(v * slab, slab), slab)
        return jnp.dot(
            sel[t, rows, :sources], tokg[p][...].reshape(sources, width),
            preferred_element_type=F32,
        )

    def arrival(p, u, v):
        return xc.at[u, v, :, pl.ds(PIECES[p][1], PIECES[p][2])]

    for trio in TRIOS:
        for p in trio:
            for d in range(SIDE):
                m_copies[p, d].wait_recv()
        if trio == TRIOS[0]:
            pl.semaphore_wait(ready.at[1], 3 * len(LINE))
        x_copies.update(exchange(trio, select, arrival, x_send, x_recv))
        if trio != TRIOS[-1]:
            for p in TRIOS[TRIOS.index(trio) + 1]:
                forward(p)

    lane = lax.broadcasted_iota(jnp.int32, (1, total), 1)
    slot_at = lane
    for q in range(1, SIDE * SIDE):
        slot_at = jnp.where(lane >= q * group, lane - q * group, slot_at)
    slot_at = slot_at.astype(F32)
    for t in range(3):
        def weigh(s, _):
            expand = lambda w: lax.dot_general(
                kw_in[t, s, w], spread[...], (((0,), (0,)), ((), ())),
                preferred_element_type=F32,
            )
            chosen = expand(0) + (s * slots).astype(F32) == slot_at
            value = jnp.where(chosen, expand(1), 0.0).astype(BF16)
            o, l = s // SIDE, s % SIDE
            return value

        def weigh_all(l, _):
            for o in range(2):
                rows = pl.ds(pl.multiple_of((o * SIDE + l) * tokens, tokens), tokens)
                sel[t, rows, :] = weigh(2 * l + o, 0)
            return 0

        lax.fori_loop(0, SIDE, weigh_all, 0)

    def arrive(p):
        for i, j in PEERS:
            x_copies[p, i, j].wait()

    def reorder(p, i):
        t, first, width = PIECES[p]
        block = xc.at[i] if t == 1 else xc.at[:, i]
        columns = pl.ds(first, width)
        res = jnp.dot(
            swap[...], block[:, :, columns].reshape(slab, width), preferred_element_type=F32
        )
        block[:, :, columns] = res.astype(BF16).reshape(SIDE, group, width)

    def reorder_all(p):
        def one(i, _):
            reorder(p, i)
            return 0

        lax.fori_loop(0, SIDE, one, 0)

    f_tile = 256
    m_rows = 2 * slab

    def first_half(k, _):
        f = pl.multiple_of(k * f_tile, f_tile)
        for m in range(2):
            x = xc[2 * m:2 * m + 2, :, :, :HALF].reshape(m_rows, HALF)
            rows = slice(m * m_rows, (m + 1) * m_rows)
            acc[rows, pl.ds(f, f_tile)] = jnp.dot(
                x, wg[:HALF, pl.ds(f, f_tile)], preferred_element_type=F32
            )
            acc[rows, pl.ds(hidden + f, f_tile)] = jnp.dot(
                x, wu[:HALF, pl.ds(f, f_tile)], preferred_element_type=F32
            )
        return 0

    def reorder_hidden(t, i):
        src = hid.at[i] if t == 1 else hid.at[:, i]
        dst = hidp.at[t - 1, i] if t == 1 else hidp.at[t - 1, :, i]
        res = jnp.dot(swap[...], src[...].reshape(slab, hidden), preferred_element_type=F32)
        dst[...] = res.astype(BF16).reshape(SIDE, group, hidden)

    def second_half(v):
        reorder(TRIOS[2][1], v)
        rows = pl.ds(pl.multiple_of(v * slab, slab), slab)

        def one(k, _):
            f = pl.multiple_of(k * f_tile, f_tile)
            x = xc[v, :, :, HALF:]
            x = x.reshape(slab, x.shape[-1])
            gate = acc[rows, pl.ds(f, f_tile)] + jnp.dot(
                x, wg[HALF:, pl.ds(f, f_tile)], preferred_element_type=F32
            )
            up = acc[rows, pl.ds(hidden + f, f_tile)] + jnp.dot(
                x, wu[HALF:, pl.ds(f, f_tile)], preferred_element_type=F32
            )
            value = (gate / (1.0 + jnp.exp(-gate)) * up).astype(BF16)
            hid[v, :, :, pl.ds(f, f_tile)] = value.reshape(SIDE, group, f_tile)
            return 0

        lax.fori_loop(0, hidden // f_tile, one, 0)
        reorder_hidden(1, v)

    for p in TRIOS[0] + TRIOS[1]:
        arrive(p)
        if PIECES[p][0] > 0:
            reorder_all(p)
    for copy in load_w:
        copy.wait()
    lax.fori_loop(0, hidden // f_tile, first_half, 0)
    arrive(TRIOS[2][2])
    reorder_all(TRIOS[2][2])
    for p in TRIOS[2][:2]:
        arrive(p)

    y_copies = {}

    def down(p, v):
        t, first, width = PIECES[p]
        source = hid if t == 0 else hidp.at[t - 1]
        return jnp.dot(
            source[v].reshape(slab, hidden), wd[:, first:first + width],
            preferred_element_type=F32,
        )

    def reorder_last(i, _):
        reorder_hidden(2, i)
        return 0

    def give_back(trio, prepare=None):
        y_copies.update(
            exchange(trio, down, lambda p, u, v: yr[p].at[u, v], y_send, y_recv, prepare)
        )

    give_back(RETURNS[0][:2], second_half)
    lax.fori_loop(0, SIDE, reorder_last, 0)
    give_back(RETURNS[0][2:])
    for trio in RETURNS[1:]:
        give_back(trio)

    for copy in l_copies.values():
        copy.wait_send()
    for copy in m_copies.values():
        copy.wait_send()
    p_copies, z_copies = {}, {}
    half = SIDE * tokens

    def share(p):
        band, first = SHARES[p]
        return acc.at[half * band:half * (band + 1), first:first + PIECES[p][2]]

    def part(p, o):
        rows = pl.ds(pl.multiple_of(o * half, half), half)
        return jnp.dot(
            sel[PIECES[p][0], rows, :], yr[p][...].reshape(total, PIECES[p][2]),
            preferred_element_type=F32,
        )

    def combine(trio):
        for p in trio:
            for i, j in PEERS:
                y_copies[p, i, j].wait()
            tokg[p][:, 0] = part(p, 1 - core).astype(BF16).reshape(SIDE, tokens, PIECES[p][2])
            copy = remote(
                tokg[p].at[:, 0], pr[p], p_send.at[p], p_recv.at[p], device((0, 0, 0), 1 - core)
            )
            copy.start()
            p_copies[p] = copy
        for p in trio:
            share(p)[...] = part(p, core)

    def reduce_cores(p):
        t, first, width = PIECES[p]
        p_copies[p].wait()
        both = share(p)[...] + pr[p][...].reshape(half, width).astype(F32)
        tokg[p][:, 1] = both.astype(BF16).reshape(SIDE, tokens, width)
        for d in LINE:
            copy = remote(
                tokg[p].at[near[t][d], 1], zr[p].at[d - 1],
                z_send.at[p, d], z_recv.at[p, d], device(on_line(t, d), core),
            )
            copy.start()
            z_copies[p, d] = copy

    def finish(p):
        t, first, width = PIECES[p]
        result = share(p)[pl.ds(pl.multiple_of(here[t] * tokens, tokens), tokens), :]
        result = result + pr[p][here[t]].astype(F32)
        for d in LINE:
            z_copies[p, d].wait()
        for d in range(1, SIDE):
            result = result + zr[p][d - 1].astype(F32)
        out_ref[:, first:first + width] = result.astype(BF16)

    for k, trio in enumerate(RETURNS):
        combine(trio)
        for p in trio:
            reduce_cores(p)
        if k == 1:
            for p in RETURNS[0]:
                finish(p)
    for trio in RETURNS[1:]:
        for p in trio:
            finish(p)


def body(tokens, expert_ids, gate_probs, w_gate, w_up, w_down):
    count, choices = expert_ids.shape
    width = tokens.shape[1]
    hidden = w_gate.shape[2]
    slots = 10
    group = 2 * SIDE * slots
    total = SIDE * SIDE * group
    n = len(PIECES)
    any_spec = pl.BlockSpec(memory_space=pl.ANY)
    dma = pltpu.SemaphoreType.DMA
    widths = [w for _, _, w in PIECES]
    scratch = (
        [pltpu.VMEM((SIDE, 2, count, w), BF16) for w in widths]
        + [pltpu.VMEM((SIDE, SIDE, group, w), BF16) for w in widths]
        + [pltpu.VMEM((SIDE, SIDE, group, w), BF16) for w in widths]
        + [pltpu.VMEM((SIDE, count, w), BF16) for w in widths]
        + [pltpu.VMEM((SIDE - 1, count, w), BF16) for w in widths]
        + [
            pltpu.VMEM((choices, count), jnp.int32),
            pltpu.VMEM((choices, count), F32),
            pltpu.VMEM((width, hidden), BF16),
            pltpu.VMEM((width, hidden), BF16),
            pltpu.VMEM((hidden, width), BF16),
            pltpu.VMEM((3, SIDE, 2, 2, 16, count), BF16),
            pltpu.VMEM((3, 2 * SIDE, 2, 16, count), BF16),
            pltpu.VMEM((16, count), F32),
            pltpu.VMEM((3, total, total), BF16),
            pltpu.VMEM((SIDE * group, SIDE * group), BF16),
            pltpu.VMEM((16, total), BF16),
            pltpu.VMEM((SIDE, SIDE, group, width), BF16),
            pltpu.VMEM((total, 2 * hidden), F32),
            pltpu.VMEM((SIDE, SIDE, group, hidden), BF16),
            pltpu.VMEM((2, SIDE, SIDE, group, hidden), BF16),
            dma((5 + n,)),
            pltpu.SemaphoreType.REGULAR((2,)),
            dma((3, SIDE, 2)), dma((3, SIDE, 2)),
            dma((n, SIDE)), dma((n, SIDE)),
            dma((n, SIDE)), dma((n, SIDE)),
            dma((n, SIDE, SIDE)), dma((n, SIDE, SIDE)),
            dma((n, SIDE, SIDE)), dma((n, SIDE, SIDE)),
            dma((n,)), dma((n,)),
            dma((n, SIDE)), dma((n, SIDE)),
        ]
    )
    return pl.pallas_call(
        functools.partial(moe_kernel, slots),
        out_shape=jax.ShapeDtypeStruct((count, width), BF16),
        in_specs=[any_spec] * 6,
        out_specs=pl.BlockSpec(memory_space=pltpu.VMEM),
        scratch_shapes=scratch,
        compiler_params=pltpu.CompilerParams(
            collective_id=0, has_side_effects=True, vmem_limit_bytes=67043328
        ),
    )(expert_ids.T, gate_probs.T, tokens, w_gate, w_up, w_down)


def solution(mesh):
    in_specs = (
        P(("row", "col"), None),
        P(("row", "col"), None),
        P(("row", "col"), None),
        P(("row", "col"), None, None),
        P(("row", "col"), None, None),
        P(("row", "col"), None, None),
    )
    out_specs = P(("row", "col"), None)
    return jax.shard_map(body, mesh=mesh, in_specs=in_specs, out_specs=out_specs, check_vma=False)
```
